32 devices in a mesh: gx: 8 (over z, x), gy: 4 (over y, core).
Axes of the slice: x: 2, y: 2, z: 4, core: 2. Of those that a mesh axis runs over, the one named last changes fastest.
Arguments:
- velocity: float32 [3, 64, 256, 256], P(None, 'gx', 'gy'), may hold values from -10 to 10
Outputs:
- coefficient: float32 [256], P('gy')
- viscosity: float32 [64, 256, 256], P('gx', 'gy')
The draws below stay inside these ranges and needn't reach their ends.
All inputs are finite; a program needn't handle non-finite values.
Results may differ from the reference program's by a relative error of at most 0.00002.
Values sent between devices are 32-bit elements; how exact they have to be, the bound alone decides.
A program may use at most 64 MiB of HBM per device.

```python
import jax
import jax.numpy as jnp
from jax import lax

NZ = 256
NX = 64
NY = 256


def draw_velocity(key, part):
    noise_key = jax.random.fold_in(key, 0)
    stream_pos = jnp.arange(NX, dtype=jnp.float32) / NX
    wall_pos = (jnp.arange(NY, dtype=jnp.float32) + 0.5) / NY
    amplitude = (0.5 + stream_pos)[:, None, None] * (0.5 + wall_pos)[None, :, None]
    fluctuation = jax.random.normal(noise_key, (3, NX, NY, NZ), jnp.float32)
    mean_flow = 6.0 * wall_pos * (1.0 - wall_pos)
    mean_field = jnp.stack([mean_flow, 0.0 * mean_flow, 0.0 * mean_flow])
    velocity_field = amplitude[None] * fluctuation + mean_field[:, None, :, None]
    return jnp.clip(velocity_field, -10.0, 10.0)


def setup_inputs(seed: int = 0) -> dict:
    arg_keys = jax.random.split(jax.random.key(seed), 2)
    velocity = draw_velocity(jax.random.fold_in(arg_keys[1], 71), 0)
    return {"velocity": velocity}


step_stream = 2.0
step_wall = 0.5
step_span = 1.0
clip_high = 0.1
weights = (1.0, 1.0, 1.0, 2.0, 2.0, 2.0)
index_pairs = ((0, 0), (1, 1), (2, 2), (0, 1), (0, 2), (1, 2))

def strain_inner(padded):
    grad_stream = (padded[:, 2:, 1:-1] - padded[:, :-2, 1:-1]) * (0.5 / step_stream)
    grad_wall = (padded[:, 1:-1, 2:] - padded[:, 1:-1, :-2]) * (0.5 / step_wall)
    centre = padded[:, 1:-1, 1:-1]
    grad_span = (jnp.roll(centre, -1, 3) - jnp.roll(centre, 1, 3)) * (0.5 / step_span)
    gradients = (grad_stream, grad_wall, grad_span)
    return jnp.stack([0.5 * (gradients[second][first] + gradients[first][second]) for first, second in index_pairs])

def weight_column():
    return jnp.asarray(weights, jnp.float32).reshape(6, 1, 1, 1)

def magnitude(strain):
    return jnp.sqrt(2.0 * lax.optimization_barrier(jnp.sum(weight_column() * strain * strain, axis=0)))

def test_filter(field):
    smoothed = 0.25 * field[:, :-2] + 0.5 * field[:, 1:-1] + 0.25 * field[:, 2:]
    return 0.25 * jnp.roll(smoothed, 1, 3) + 0.5 * smoothed + 0.25 * jnp.roll(smoothed, -1, 3)

def plane_sums(velocity_pad, stress_pad, filtered_pad):
    strain_hat = strain_inner(filtered_pad)
    magnitude_hat = magnitude(strain_hat)
    row_values = velocity_pad[:, :, 1:-1]
    products = jnp.stack([row_values[first] * row_values[second] for first, second in index_pairs])
    product_hat = test_filter(products)
    centre = filtered_pad[:, 1:-1, 1:-1]
    leonard = product_hat - jnp.stack([centre[first] * centre[second] for first, second in index_pairs])
    trace_third = (leonard[0] + leonard[1] + leonard[2]) / 3.0
    leonard = jnp.concatenate([leonard[:3] - trace_third[None], leonard[3:]])
    model_tensor = 2.0 * (test_filter(stress_pad) - 4.0 * magnitude_hat[None] * strain_hat)
    numerator = lax.optimization_barrier(jnp.sum(weight_column() * leonard * model_tensor, axis=(0, 1, 3)))
    denominator = lax.optimization_barrier(jnp.sum(weight_column() * model_tensor * model_tensor, axis=(0, 1, 3)))
    return (numerator, denominator)

def wrap_stream(field):
    return jnp.concatenate([field[:, -1:], field, field[:, :1]], axis=1)

def pad_walls(field):
    return jnp.pad(field, ((0, 0), (0, 0), (1, 1), (0, 0)))

def reference(velocity):
    velocity_pad = pad_walls(wrap_stream(velocity))
    strain = strain_inner(velocity_pad)
    strength = magnitude(strain)
    stress = strength[None] * strain
    filtered = test_filter(velocity_pad[:, :, 1:-1])
    filtered_pad = pad_walls(wrap_stream(filtered))
    stress_pad = wrap_stream(stress)
    numerator, denominator = plane_sums(velocity_pad, stress_pad, filtered_pad)
    raw_profile = jnp.clip(numerator / denominator, 0.0, clip_high)
    rim_values = jnp.concatenate([raw_profile[:1], raw_profile, raw_profile[-1:]])
    smooth = 0.25 * rim_values[:-2] + 0.5 * raw_profile + 0.25 * rim_values[2:]
    return (smooth, smooth[None, :, None] * strength)
```

```python
import functools

import jax
import jax.numpy as jnp
from jax import lax
from jax.experimental import pallas as pl
from jax.experimental.pallas import tpu as pltpu
from jax.sharding import PartitionSpec as P

clip_high = 0.1
pairs = ((0, 0), (1, 1), (2, 2), (0, 1), (0, 2), (1, 2))
MESH = pl.DeviceIdType.MESH
HALO = 3


def tile(index):
    return pl.ds(pl.multiple_of(index * 8, 8), 8)


def roll_next(value):
    return pltpu.roll(value, value.shape[1] - 1, 1)


def roll_prev(value):
    return pltpu.roll(value, 1, 1)


def filter_span(value):
    return (roll_next(value) + roll_prev(value)) + 2.0 * value


def slope_span(value):
    return roll_next(value) - roll_prev(value)


def slope_wall(ref, comp, row, t, here):
    rows = lax.broadcasted_iota(jnp.int32, here.shape, 0)
    below = ref[comp, row, tile(t - 1), :]
    above = ref[comp, row, tile(t + 1), :]
    up = pltpu.roll(jnp.where(rows == 0, above, here), 7, 0)
    down = pltpu.roll(jnp.where(rows == 7, below, here), 1, 0)
    return up - down


def strain4(ref, row, t, slope=None):
    here = [ref[c, row, tile(t), :] for c in range(3)]
    dx = [ref[c, row + 1, tile(t), :] - ref[c, row - 1, tile(t), :] for c in range(3)]
    dy = [slope_wall(ref, c, row, t, here[c]) for c in range(3)]
    if slope is None:
        dz = [slope_span(here[c]) for c in range(3)]
    else:
        dz = [slope[c, row, tile(t), :] for c in range(3)]
    s = (
        dx[0],
        4.0 * dy[1],
        2.0 * dz[2],
        2.0 * dy[0] + 0.5 * dx[1],
        dz[0] + 0.5 * dx[2],
        dz[1] + 2.0 * dy[2],
    )
    diag = s[0] * s[0] + s[1] * s[1] + s[2] * s[2]
    off = s[3] * s[3] + s[4] * s[4] + s[5] * s[5]
    return here, s, diag + 2.0 * off


def kernel(n, m, nx, ny, shifts, u_hbm, strength, coef_ref, u, w, v, d, g, accn, accd,
           mine, mine_ends, gather, own_sem, xs_send, xs_recv, ys_send, ys_recv,
           c_send, c_recv, g_send, g_recv, ready, ring):
    nt = ny // 8
    edge_lo, edge_hi = HALO, HALO + nx - 1
    gx = lax.axis_index("gx")
    gy = lax.axis_index("gy")
    left, right = lax.rem(gx + n - 1, n), lax.rem(gx + 1, n)
    not_low, not_high = gy > 0, gy < m - 1
    begins, ends_ring = gx == 0, gx == n - 1
    lanes = mine.shape[-1]
    shifting = any(shifts)

    def shift_at(index):
        value = jnp.int32(shifts[0])
        for i in range(1, n):
            if shifts[i] != shifts[0]:
                value = jnp.where(index == i, jnp.int32(shifts[i]), value)
        return value

    gains = (shift_at(left), -shift_at(gx)) if shifting else (0, 0)
    more = [jnp.maximum(x, 0) if shifting else 0 for x in gains]
    fewer = [jnp.maximum(-x, 0) if shifting else 0 for x in gains]

    own = [
        pltpu.make_async_copy(
            u_hbm.at[:, a:b, :, :], u.at[:, edge_lo + a:edge_lo + b, 8:8 + ny, :], own_sem.at[k]
        )
        for k, (a, b) in enumerate(((0, 1), (nx - 1, nx), (1, nx - 1)))
    ]
    for copy in own:
        copy.start()

    def signal(semaphore, to_x, to_y):
        pl.semaphore_signal(semaphore, inc=1, device_id=(to_x, to_y), device_id_type=MESH)

    barrier = pltpu.get_barrier_semaphore()

    @pl.when(jnp.logical_not(ends_ring))
    def _():
        signal(barrier, right, gy)

    @pl.when(begins)
    def _():
        signal(barrier, left, gy)

    @pl.when(not_high)
    def _():
        signal(barrier, gx, gy + 1)

    earlier = [jnp.where(x, 1, 0) for x in (gx > 0, ends_ring, not_low)]
    greeted = earlier[0] + earlier[1] + earlier[2]

    @pl.when(greeted > 0)
    def _():
        pl.semaphore_wait(barrier, greeted)

    @pl.when(gx > 0)
    def _():
        signal(ready.at[0], left, gy)

    @pl.when(ends_ring)
    def _():
        signal(ready.at[1], right, gy)

    @pl.when(not_low)
    def _():
        signal(ready.at[2], gx, gy - 1)

    ends = jnp.where(not_low, 1, 0) + jnp.where(not_high, 1, 0)
    rounds = n // 2 - 1

    def to_sides(semaphore):
        for side in (left, right):
            signal(semaphore, side, gy)

    def to_ends(semaphore):
        @pl.when(not_low)
        def _():
            signal(semaphore, gx, gy - 1)

        @pl.when(not_high)
        def _():
            signal(semaphore, gx, gy + 1)

    def open_round(k):
        if k < rounds:
            to_sides(ring.at[k])

    def close_round(k):
        if k < rounds:
            pl.semaphore_wait(ring.at[k], 2)

    def order(i):
        return jnp.where(i == 0, nt, i)

    def halo_row(side, k):
        return edge_lo - k if side == 0 else edge_hi + k

    def x_copy(side, k, t):
        src = halo_row(side, 1 - k)
        dst = halo_row(1 - side, k)
        return pltpu.make_async_remote_copy(
            src_ref=u.at[:, src:src + 1, tile(t), :],
            dst_ref=u.at[:, dst:dst + 1, tile(t), :],
            send_sem=xs_send.at[side, k - 1, t - 1],
            recv_sem=xs_recv.at[1 - side, k - 1, t - 1],
            device_id=(left if side == 0 else right, gy),
            device_id_type=MESH,
        )

    def all_sends(side, k, act):
        def each(i, carry):
            act(x_copy(side, k, order(i)))
            return carry

        low = nt - fewer[side] if k == 3 else 0
        high = nt - more[side] if k == 2 else nt
        if k < 3 or shifting:
            lax.fori_loop(low, high, each, 0)

    def send_x(side, k):
        all_sends(side, k, lambda copy: copy.start())

    def y_copy(side):
        src = 8 if side == 0 else ny
        dst = ny + 8 if side == 0 else 0
        return pltpu.make_async_remote_copy(
            src_ref=u.at[:, edge_lo:edge_lo + nx, src:src + 8, :],
            dst_ref=u.at[:, edge_lo:edge_lo + nx, dst:dst + 8, :],
            send_sem=ys_send.at[side],
            recv_sem=ys_recv.at[side],
            device_id=(gx, gy - 1 if side == 0 else gy + 1),
            device_id_type=MESH,
        )

    def c_copy(side, end):
        row = halo_row(side, 1)
        src = 8 if end == 0 else ny
        dst = ny + 8 if end == 0 else 0
        return pltpu.make_async_remote_copy(
            src_ref=u.at[:, row:row + 1, src:src + 8, :],
            dst_ref=u.at[:, row:row + 1, dst:dst + 8, :],
            send_sem=c_send.at[side, end],
            recv_sem=c_recv.at[side, end],
            device_id=(gx, gy - 1 if end == 0 else gy + 1),
            device_id_type=MESH,
        )

    own[0].wait()

    @pl.when(gx > 0)
    def _():
        send_x(0, 1)

    own[1].wait()

    @pl.when(ends_ring)
    def _():
        send_x(1, 1)

    own[2].wait()

    @pl.when(gx > 0)
    def _():
        send_x(0, 2)
        send_x(0, 3)

    @pl.when(ends_ring)
    def _():
        send_x(1, 2)
        send_x(1, 3)

    @pl.when(not_low)
    def _():
        y_copy(0).start()

    @pl.when(jnp.logical_not(ends_ring))
    def _():
        pl.semaphore_wait(ready.at[0], 1)
        for k in (1, 2, 3):
            send_x(1, k)

    @pl.when(not_high)
    def _():
        pl.semaphore_wait(ready.at[2], 1)
        y_copy(1).start()

    accn[...] = jnp.zeros_like(accn)
    accd[...] = jnp.zeros_like(accd)
    rows_all = u.shape[1]

    @pl.when(jnp.logical_not(not_low))
    def _():
        u[:, :, 0:8, :] = jnp.zeros((3, rows_all, 8, u.shape[3]), jnp.float32)

    @pl.when(jnp.logical_not(not_high))
    def _():
        u[:, :, ny + 8:ny + 16, :] = jnp.zeros((3, rows_all, 8, u.shape[3]), jnp.float32)

    def span_rows(t, rows, slopes=True):
        for c in range(3):
            for row in rows:
                here = u[c, row, tile(t), :]
                after, before = roll_next(here), roll_prev(here)
                w[c, row, tile(t), :] = (after + before) + 2.0 * here
                if slopes:
                    d[c, row, tile(t), :] = after - before

    def filtered_rows(t, rows):
        for c in range(3):
            for row in rows:
                a, b, e = (w[c, row + k, tile(t), :] for k in (-1, 0, 1))
                v[c, row, tile(t), :] = 0.25 * ((a + e) + 2.0 * b)

    def stress_row(t, row, keep):
        _, s, total = strain4(u, row, t, d)
        size = jnp.sqrt(0.125 * total)
        if keep:
            strength[row - edge_lo, tile(t - 1), :] = size
        for k in range(6):
            g[k, row, tile(t - 1), :] = size * s[k]

    def sums_row(t, row):
        centre, s, total = strain4(v, row, t)
        scale = jnp.sqrt(2.0 * total)

        def product(a, b):
            one, two, three = (near[j][a] * near[j][b] for j in range(3))
            return filter_span((one + three) + 2.0 * two)

        def stress(k):
            one, two, three = (g[k, row + j, tile(t - 1), :] for j in (-1, 0, 1))
            return filter_span((one + three) + 2.0 * two)

        near = [[u[c, row + j, tile(t), :] for c in range(3)] for j in (-1, 0, 1)]
        leonard = [product(a, b) - centre[a] * centre[b] for a, b in pairs]
        third = (leonard[0] + leonard[1] + leonard[2]) * (1.0 / 3.0)
        leonard = [x - third for x in leonard[:3]] + leonard[3:]
        model = [stress(k) - scale * s[k] for k in range(6)]
        lm = [x * y for x, y in zip(leonard, model)]
        mm = [x * x for x in model]
        num = (lm[0] + lm[1] + lm[2]) + 2.0 * (lm[3] + lm[4] + lm[5])
        den = (mm[0] + mm[1] + mm[2]) + 2.0 * (mm[3] + mm[4] + mm[5])
        return num, den

    def fold(value):
        parts = [value[:, k:k + 128] for k in range(0, value.shape[1], 128)]
        return functools.reduce(lambda x, y: x + y, parts)

    def sums(t, rows):
        both = [sums_row(t, row) for row in rows]
        num = functools.reduce(lambda x, y: x + y, [b[0] for b in both])
        den = functools.reduce(lambda x, y: x + y, [b[1] for b in both])
        accn[tile(t - 1), :] += fold(num)
        accd[tile(t - 1), :] += fold(den)

    def inner_filter(t, carry):
        span_rows(t, range(edge_lo, edge_hi + 1))
        filtered_rows(t, range(edge_lo + 1, edge_hi))
        return carry

    lax.fori_loop(1, nt + 1, inner_filter, 0)

    @pl.when(not_high)
    def _():
        y_copy(0).wait_recv()

    @pl.when(not_low)
    def _():
        y_copy(1).wait_recv()

    def end_filter(i, carry):
        return inner_filter(i * (nt + 1), carry)

    lax.fori_loop(0, 2, end_filter, 0)

    half = (nx - 2) // 2

    def inner_stress(i, carry):
        t = i // half + 1
        row = edge_lo + 1 + 2 * lax.rem(i, half)
        stress_row(t, row, True)
        stress_row(t, row + 1, True)
        return carry

    lax.fori_loop(0, nt * half, inner_stress, 0)

    def inner_sums(t, carry):
        sums(t, range(edge_lo + 2, edge_hi - 1))
        return carry

    lax.fori_loop(1, nt + 1, inner_sums, 0)

    @pl.when(begins)
    def _():
        pl.semaphore_wait(ready.at[1], 1)
        for k in (1, 2, 3):
            send_x(0, k)

    open_round(0)

    def step(side, k, t):
        x_copy(1 - side, k, t).wait_recv()
        new, middle, old = (halo_row(side, k - j) for j in range(3))
        span_rows(t, (new,), k == 1 or shifting and k == 2)
        filtered_rows(t, (middle,))
        stress_row(t, middle, k == 1)
        sums(t, (old,))

    def near(i, carry):
        t = order(i)
        for side in range(2):
            step(side, 1, t)

            @pl.when(jnp.logical_and(i == 0, not_high))
            def _():
                c_copy(side, 1).start()

            @pl.when(jnp.logical_and(i == 1, not_low))
            def _():
                c_copy(side, 0).start()

        return carry

    lax.fori_loop(0, nt, near, 0)
    close_round(0)
    open_round(1)

    for side in range(2):
        @pl.when(not_high)
        def _():
            c_copy(side, 0).wait_recv()

        @pl.when(not_low)
        def _():
            c_copy(side, 1).wait_recv()

    def corners(i, carry):
        t = i * (nt + 1)
        for side in range(2):
            span_rows(t, (halo_row(side, 1),), False)
            filtered_rows(t, (halo_row(side, 0),))
        return carry

    lax.fori_loop(0, 2, corners, 0)
    close_round(1)
    open_round(2)

    def far(k):
        def run(i, carry):
            t = order(i)
            for side in range(2):
                if not shifting:
                    step(side, k, t)
                    continue
                wanted = i < nt - fewer[side] if k == 2 else i >= nt - more[side]

                @pl.when(wanted)
                def _():
                    step(side, k, t)

            return carry

        return run

    lax.fori_loop(0, 2, far(2), 0)
    close_round(2)

    def later_round(k, carry):
        to_sides(ring.at[k])
        pl.semaphore_wait(ring.at[k], 2)
        return carry

    if rounds > 3:
        lax.fori_loop(3, rounds, later_round, 0)
    to_ends(ring.at[n // 2])

    def column_sums(ref):
        ref[0:1, :] = jnp.sum(accn[...].T, axis=0, keepdims=True)
        ref[1:2, :] = jnp.sum(accd[...].T, axis=0, keepdims=True)

    def g_copy(kind, to_x, to_y):
        return pltpu.make_async_remote_copy(
            src_ref=mine if kind == 0 else mine_ends,
            dst_ref=gather.at[kind, gx],
            send_sem=g_send.at[kind],
            recv_sem=g_recv.at[kind],
            device_id=(to_x, to_y),
            device_id_type=MESH,
        )

    def g_all(kind):
        count = n - 1 if kind == 0 else n
        part = gather.at[kind, 0:count]
        return pltpu.make_async_remote_copy(
            src_ref=part,
            dst_ref=part,
            send_sem=g_send.at[kind],
            recv_sem=g_recv.at[kind],
            device_id=(right, gy),
            device_id_type=MESH,
        )

    column_sums(mine_ends)
    pl.semaphore_wait(ring.at[n // 2], ends)

    def send_ends(i, carry):
        @pl.when(not_low)
        def _():
            g_copy(2, i, gy - 1).start()

        @pl.when(not_high)
        def _():
            g_copy(1, i, gy + 1).start()

        return carry

    lax.fori_loop(0, n, send_ends, 0)

    lax.fori_loop(2, nt, far(2), 0)
    if shifting:
        top = functools.reduce(jnp.maximum, more)
        lax.fori_loop(nt - top, nt, far(3), 0)

    column_sums(mine)
    def drain():
        for side in range(2):
            for k in (1, 2, 3):
                all_sends(side, k, lambda copy: copy.wait_send())

    def send(i, carry):
        g_copy(0, lax.rem(gx + i, n), gy).start()
        return carry

    lax.fori_loop(1, n, send, 0)
    gather[0, gx] = mine[...]
    drain()
    g_all(0).wait_recv()

    @pl.when(not_low)
    def _():
        g_all(1).wait_recv()

    @pl.when(not_high)
    def _():
        g_all(2).wait_recv()

    def profile(kind):
        def add(i, total):
            return total + gather[kind, i]

        total = lax.fori_loop(0, n, add, jnp.zeros((2, lanes), jnp.float32))
        return jnp.clip(2.0 * (total[0:1] / total[1:2]), 0.0, clip_high)

    raw = profile(0)
    where = lax.broadcasted_iota(jnp.int32, (1, lanes), 1)
    first = where == 0
    last = where == ny - 1
    under = jnp.where(first, raw, pltpu.roll(raw, 1, 1))
    over = jnp.where(last, raw, pltpu.roll(raw, lanes - 1, 1))
    low_raw = pltpu.roll(profile(1), (lanes + 1 - ny) % lanes, 1)
    high_raw = pltpu.roll(profile(2), ny - 1, 1)
    under = jnp.where(jnp.logical_and(first, not_low), low_raw, under)
    over = jnp.where(jnp.logical_and(last, not_high), high_raw, over)
    coef_ref[...] = 0.25 * under + 0.5 * raw + 0.25 * over

    for side in range(2):
        @pl.when(not_low)
        def _():
            c_copy(side, 0).wait_send()

        @pl.when(not_high)
        def _():
            c_copy(side, 1).wait_send()

    @pl.when(not_low)
    def _():
        y_copy(0).wait_send()

    @pl.when(not_high)
    def _():
        y_copy(1).wait_send()

    g_all(0).wait_send()

    @pl.when(not_low)
    def _():
        g_all(2).wait_send()

    @pl.when(not_high)
    def _():
        g_all(1).wait_send()


def local(n, m, shifts, velocity):
    _, nx, ny, nz = velocity.shape
    lanes = -(-ny // 128) * 128
    nt = ny // 8
    f32 = jnp.float32
    strength, coef = pl.pallas_call(
        functools.partial(kernel, n, m, nx, ny, shifts),
        out_shape=(
            jax.ShapeDtypeStruct((nx, ny, nz), f32),
            jax.ShapeDtypeStruct((1, lanes), f32),
        ),
        in_specs=[pl.BlockSpec(memory_space=pltpu.HBM)],
        out_specs=(
            pl.BlockSpec(memory_space=pltpu.VMEM),
            pl.BlockSpec(memory_space=pltpu.VMEM),
        ),
        scratch_shapes=[
            pltpu.VMEM((3, nx + 2 * HALO, ny + 16, nz), f32),
            pltpu.VMEM((3, nx + 2 * HALO, ny + 16, nz), f32),
            pltpu.VMEM((3, nx + 2 * HALO, ny + 16, nz), f32),
            pltpu.VMEM((3, nx + 2 * HALO, ny + 16, nz), f32),
            pltpu.VMEM((6, nx + 2 * HALO, ny, nz), f32),
            pltpu.VMEM((lanes, 128), f32),
            pltpu.VMEM((lanes, 128), f32),
            pltpu.VMEM((2, lanes), f32),
            pltpu.VMEM((2, lanes), f32),
            pltpu.VMEM((3, n, 2, lanes), f32),
            pltpu.SemaphoreType.DMA((3,)),
            pltpu.SemaphoreType.DMA((2, HALO, nt)),
            pltpu.SemaphoreType.DMA((2, HALO, nt)),
            pltpu.SemaphoreType.DMA((2,)),
            pltpu.SemaphoreType.DMA((2,)),
            pltpu.SemaphoreType.DMA((2, 2)),
            pltpu.SemaphoreType.DMA((2, 2)),
            pltpu.SemaphoreType.DMA((3,)),
            pltpu.SemaphoreType.DMA((3,)),
            pltpu.SemaphoreType.REGULAR((3,)),
            pltpu.SemaphoreType.REGULAR((n // 2 + 1,)),
        ],
        compiler_params=pltpu.CompilerParams(
            collective_id=0, has_side_effects=True, vmem_limit_bytes=32 * 1024 * 1024
        ),
    )(pltpu.with_memory_space_constraint(velocity, pltpu.HBM))
    smooth = coef[0, :ny]
    return (smooth, smooth[None, :, None] * strength)


def solution(mesh):
    n, m = mesh.shape["gx"], mesh.shape["gy"]
    shifts = (0,) * n
    return jax.shard_map(
        functools.partial(local, n, m, shifts),
        mesh=mesh,
        in_specs=(P(None, "gx", "gy", None),),
        out_specs=(P("gy"), P("gx", "gy", None)),
        check_vma=False,
    )
```

```python
import functools

import jax
import jax.numpy as jnp
from jax import lax
from jax.experimental import pallas as pl
from jax.experimental.pallas import tpu as pltpu
from jax.sharding import PartitionSpec as P

clip_high = 0.1
pairs = ((0, 0), (1, 1), (2, 2), (0, 1), (0, 2), (1, 2))
MESH = pl.DeviceIdType.MESH
HALO = 3


def tile(index):
    return pl.ds(pl.multiple_of(index * 8, 8), 8)


def roll_next(value):
    return pltpu.roll(value, value.shape[1] - 1, 1)


def roll_prev(value):
    return pltpu.roll(value, 1, 1)


def filter_span(value):
    return (roll_next(value) + roll_prev(value)) + 2.0 * value


def slope_span(value):
    return roll_next(value) - roll_prev(value)


def slope_wall(ref, comp, row, t, here):
    rows = lax.broadcasted_iota(jnp.int32, here.shape, 0)
    below = ref[comp, row, tile(t - 1), :]
    above = ref[comp, row, tile(t + 1), :]
    up = pltpu.roll(jnp.where(rows == 0, above, here), 7, 0)
    down = pltpu.roll(jnp.where(rows == 7, below, here), 1, 0)
    return up - down


def strain4(ref, row, t, slope=None):
    here = [ref[c, row, tile(t), :] for c in range(3)]
    dx = [ref[c, row + 1, tile(t), :] - ref[c, row - 1, tile(t), :] for c in range(3)]
    dy = [slope_wall(ref, c, row, t, here[c]) for c in range(3)]
    if slope is None:
        dz = [slope_span(here[c]) for c in range(3)]
    else:
        dz = [slope[c, row, tile(t), :] for c in range(3)]
    s = (
        dx[0],
        4.0 * dy[1],
        2.0 * dz[2],
        2.0 * dy[0] + 0.5 * dx[1],
        dz[0] + 0.5 * dx[2],
        dz[1] + 2.0 * dy[2],
    )
    diag = s[0] * s[0] + s[1] * s[1] + s[2] * s[2]
    off = s[3] * s[3] + s[4] * s[4] + s[5] * s[5]
    return here, s, diag + 2.0 * off


def cuts_of(nt):
    edges = [0, min(3, nt)]
    while nt - edges[-1] > 1:
        edges.append(min(edges[-1] + 2, nt - 1))
    if edges[-1] < nt:
        edges.append(nt)
    return edges


def kernel(n, m, nx, ny, shifts, u_hbm, strength, coef_ref, u, w, v, d, g, accn, accd,
           mine, mine_ends, gather, own_sem, xs_send, xs_recv, y_send, y_recv,
           c_recv, g_send, g_recv, ready, ring):
    nt = ny // 8
    edge_lo, edge_hi = HALO, HALO + nx - 1
    gx = lax.axis_index("gx")
    gy = lax.axis_index("gy")
    left, right = lax.rem(gx + n - 1, n), lax.rem(gx + 1, n)
    not_low, not_high = gy > 0, gy < m - 1
    begins, closes = gx == 0, gx == n - 1
    lanes = mine.shape[-1]
    shifting = any(shifts)
    cuts = cuts_of(nt)
    pieces = len(cuts) - 1
    moved = cuts[max(pieces - 2, 1)]

    def shift_at(index):
        value = jnp.int32(shifts[0])
        for i in range(1, n):
            if shifts[i] != shifts[0]:
                value = jnp.where(index == i, jnp.int32(shifts[i]), value)
        return value

    gains = (shift_at(left), -shift_at(gx)) if shifting else (0, 0)

    own = [
        pltpu.make_async_copy(
            u_hbm.at[:, a:b, :, :], u.at[:, edge_lo + a:edge_lo + b, 8:8 + ny, :], own_sem.at[k]
        )
        for k, (a, b) in enumerate(((0, 1), (nx - 1, nx), (1, nx - 1)))
    ]
    for copy in own:
        copy.start()

    def signal(semaphore, to_x, to_y):
        pl.semaphore_signal(semaphore, inc=1, device_id=(to_x, to_y), device_id_type=MESH)

    barrier = pltpu.get_barrier_semaphore()

    @pl.when(jnp.logical_not(closes))
    def _():
        signal(barrier, right, gy)

    @pl.when(begins)
    def _():
        signal(barrier, left, gy)

    @pl.when(not_high)
    def _():
        signal(barrier, gx, gy + 1)

    earlier = [jnp.where(x, 1, 0) for x in (gx > 0, closes, not_low)]
    greeted = earlier[0] + earlier[1] + earlier[2]

    @pl.when(greeted > 0)
    def _():
        pl.semaphore_wait(barrier, greeted)

    @pl.when(gx > 0)
    def _():
        signal(ready.at[0], left, gy)

    @pl.when(closes)
    def _():
        signal(ready.at[1], right, gy)

    @pl.when(not_low)
    def _():
        signal(ready.at[2], gx, gy - 1)

    ends = jnp.where(not_low, 1, 0) + jnp.where(not_high, 1, 0)
    reaches = [2 ** k for k in range(n.bit_length()) if 2 ** k < n]

    def open_round(k):
        if k < len(reaches):
            @pl.when(gx >= reaches[k])
            def _():
                signal(ring.at[k], gx - reaches[k], gy)

            @pl.when(gx < n - reaches[k])
            def _():
                signal(ring.at[k], gx + reaches[k], gy)

    def close_round(k):
        if k < len(reaches):
            near = (gx >= reaches[k], gx < n - reaches[k])
            count = jnp.where(near[0], 1, 0) + jnp.where(near[1], 1, 0)

            @pl.when(count > 0)
            def _():
                pl.semaphore_wait(ring.at[k], count)

    def to_ends(semaphore):
        @pl.when(not_low)
        def _():
            signal(semaphore, gx, gy - 1)

        @pl.when(not_high)
        def _():
            signal(semaphore, gx, gy + 1)

    def order(i):
        return jnp.where(i == 0, nt, i)

    def halo_row(side, k):
        return edge_lo - k if side == 0 else edge_hi + k

    def x_copy(side, k, low, high, slot):
        src = halo_row(side, 1 - k)
        dst = halo_row(1 - side, k)
        return pltpu.make_async_remote_copy(
            src_ref=u.at[:, src:src + 1, 8 * low:8 * high, :],
            dst_ref=u.at[:, dst:dst + 1, 8 * low:8 * high, :],
            send_sem=xs_send.at[side],
            recv_sem=xs_recv.at[1 - side, slot],
            device_id=(left if side == 0 else right, gy),
            device_id_type=MESH,
        )

    def near_copy(side):
        return x_copy(side, 1, 1, nt + 1, 0)

    def moved_copy(side):
        return x_copy(side, 3, moved, nt, pieces + 1)

    def far_parts(p):
        if p == 0:
            return [(nt, nt + 1), (1, cuts[1])] if cuts[1] > 1 else [(nt, nt + 1)]
        return [(cuts[p], cuts[p + 1])]

    def start_far(side, p):
        def run():
            for low, high in far_parts(p):
                x_copy(side, 2, low, high, p + 1).start()

        if shifting and p >= pieces - 2:
            pl.when(gains[side] <= 0)(run)
        else:
            run()

    def start_moved(side):
        if shifting:
            @pl.when(gains[side] < 0)
            def _():
                moved_copy(side).start()

    def wait_far(side, p):
        count = cuts[p + 1] - cuts[p]
        x_copy(1 - side, 2, 1, 1 + count, p + 1).wait_recv()

    def tiles_view(count):
        rows = next(r for r in range(1, u.shape[1] + 1) if count % r == 0 and count // r <= nt + 2)
        return u.at[:, 0:rows, 0:8 * (count // rows), :]

    def drain():
        for side in range(2):
            if not shifting:
                wait_rows(side, tiles_view(nt))
                continue
            for sign, count in ((0, nt), (1, moved), (-1, 2 * nt - moved)):
                @pl.when(gains[side] == sign)
                def _():
                    wait_rows(side, tiles_view(count))

    def y_copy(side):
        src = 8 if side == 0 else ny + 7
        dst = ny + 8 if side == 0 else 7
        return pltpu.make_async_remote_copy(
            src_ref=u.at[:, edge_lo:edge_lo + nx, src:src + 1, :],
            dst_ref=u.at[:, edge_lo:edge_lo + nx, dst:dst + 1, :],
            send_sem=y_send.at[side],
            recv_sem=y_recv.at[side],
            device_id=(gx, gy - 1 if side == 0 else gy + 1),
            device_id_type=MESH,
        )

    def c_copy(side, end):
        row = halo_row(side, 1)
        src = 8 if end == 0 else ny + 7
        dst = ny + 8 if end == 0 else 7
        return pltpu.make_async_remote_copy(
            src_ref=u.at[:, row:row + 1, src:src + 1, :],
            dst_ref=u.at[:, row:row + 1, dst:dst + 1, :],
            send_sem=y_send.at[end],
            recv_sem=c_recv.at[end],
            device_id=(gx, gy - 1 if end == 0 else gy + 1),
            device_id_type=MESH,
        )

    def c_all(end, rows, semaphore):
        part = u.at[:, 0:rows, 8:9, :]
        return pltpu.make_async_remote_copy(
            src_ref=part,
            dst_ref=part,
            send_sem=y_send.at[end],
            recv_sem=semaphore,
            device_id=(gx, gy - 1 if end == 0 else gy + 1),
            device_id_type=MESH,
        )

    def wait_rows(side, part):
        pltpu.make_async_remote_copy(
            src_ref=part,
            dst_ref=part,
            send_sem=xs_send.at[side],
            recv_sem=xs_recv.at[1 - side, 0],
            device_id=(left if side == 0 else right, gy),
            device_id_type=MESH,
        ).wait_send()

    plans = (((0, 1, 2, 3), (), (), (), ()), ((), (), (0, 1, 2, 3), (), ()))
    odd = lax.rem(gy, 2) == 1

    def start_all(point, sides=(0, 1)):
        chosen = [[p for p in plan[point] if p < pieces] for plan in plans]

        def run(parts):
            for p in parts:
                for side in sides:
                    start_far(side, p)

        if chosen[0] == chosen[1]:
            run(chosen[0])
            return
        if chosen[0]:
            pl.when(jnp.logical_not(odd))(lambda: run(chosen[0]))
        if chosen[1]:
            pl.when(odd)(lambda: run(chosen[1]))

    own[0].wait()

    @pl.when(gx > 0)
    def _():
        near_copy(0).start()

    own[1].wait()

    @pl.when(closes)
    def _():
        near_copy(1).start()

    own[2].wait()

    @pl.when(not_low)
    def _():
        y_copy(0).start()

    @pl.when(jnp.logical_not(closes))
    def _():
        pl.semaphore_wait(ready.at[0], 1)
        near_copy(1).start()

    open_round(0)

    @pl.when(not_high)
    def _():
        pl.semaphore_wait(ready.at[2], 1)
        y_copy(1).start()

    accn[...] = jnp.zeros_like(accn)
    accd[...] = jnp.zeros_like(accd)
    rows_all = u.shape[1]

    @pl.when(jnp.logical_not(not_low))
    def _():
        u[:, :, 0:8, :] = jnp.zeros((3, rows_all, 8, u.shape[3]), jnp.float32)

    @pl.when(jnp.logical_not(not_high))
    def _():
        u[:, :, ny + 8:ny + 16, :] = jnp.zeros((3, rows_all, 8, u.shape[3]), jnp.float32)

    def span_rows(t, rows, slopes=True):
        for c in range(3):
            for row in rows:
                here = u[c, row, tile(t), :]
                after, before = roll_next(here), roll_prev(here)
                w[c, row, tile(t), :] = (after + before) + 2.0 * here
                if slopes:
                    d[c, row, tile(t), :] = after - before

    def filtered_rows(t, rows):
        for c in range(3):
            for row in rows:
                a, b, e = (w[c, row + k, tile(t), :] for k in (-1, 0, 1))
                v[c, row, tile(t), :] = 0.25 * ((a + e) + 2.0 * b)

    def stress_row(t, row, keep):
        _, s, total = strain4(u, row, t, d)
        size = jnp.sqrt(0.125 * total)
        if keep:
            strength[row - edge_lo, tile(t - 1), :] = size
        for k in range(6):
            g[k, row, tile(t - 1), :] = size * s[k]

    def sums_row(t, row):
        centre, s, total = strain4(v, row, t)
        scale = jnp.sqrt(2.0 * total)

        def product(a, b):
            one, two, three = (near[j][a] * near[j][b] for j in range(3))
            return filter_span((one + three) + 2.0 * two)

        def stress(k):
            one, two, three = (g[k, row + j, tile(t - 1), :] for j in (-1, 0, 1))
            return filter_span((one + three) + 2.0 * two)

        near = [[u[c, row + j, tile(t), :] for c in range(3)] for j in (-1, 0, 1)]
        leonard = [product(a, b) - centre[a] * centre[b] for a, b in pairs]
        third = (leonard[0] + leonard[1] + leonard[2]) * (1.0 / 3.0)
        leonard = [x - third for x in leonard[:3]] + leonard[3:]
        model = [stress(k) - scale * s[k] for k in range(6)]
        lm = [x * y for x, y in zip(leonard, model)]
        mm = [x * x for x in model]
        num = (lm[0] + lm[1] + lm[2]) + 2.0 * (lm[3] + lm[4] + lm[5])
        den = (mm[0] + mm[1] + mm[2]) + 2.0 * (mm[3] + mm[4] + mm[5])
        return num, den

    def fold(value):
        parts = [value[:, k:k + 128] for k in range(0, value.shape[1], 128)]
        return functools.reduce(lambda x, y: x + y, parts)

    def sums(t, rows):
        both = [sums_row(t, row) for row in rows]
        num = functools.reduce(lambda x, y: x + y, [b[0] for b in both])
        den = functools.reduce(lambda x, y: x + y, [b[1] for b in both])
        accn[tile(t - 1), :] += fold(num)
        accd[tile(t - 1), :] += fold(den)

    def inner_filter(t, carry):
        span_rows(t, range(edge_lo, edge_hi + 1))
        filtered_rows(t, range(edge_lo + 1, edge_hi))
        return carry

    lax.fori_loop(1, nt + 1, inner_filter, 0)

    @pl.when(not_high)
    def _():
        y_copy(0).wait_recv()

    @pl.when(not_low)
    def _():
        y_copy(1).wait_recv()

    def end_filter(i, carry):
        return inner_filter(i * (nt + 1), carry)

    lax.fori_loop(0, 2, end_filter, 0)

    half = (nx - 2) // 2

    def inner_stress(i, carry):
        t = i // half + 1
        row = edge_lo + 1 + 2 * lax.rem(i, half)
        stress_row(t, row, True)
        stress_row(t, row + 1, True)
        return carry

    lax.fori_loop(0, nt * half, inner_stress, 0)
    close_round(0)
    open_round(1)

    @pl.when(begins)
    def _():
        pl.semaphore_wait(ready.at[1], 1)
        near_copy(0).start()

    def inner_sums(t, carry):
        sums(t, range(edge_lo + 2, edge_hi - 1))
        return carry

    lax.fori_loop(1, nt + 1, inner_sums, 0)
    close_round(1)
    open_round(2)

    for side in range(2):
        near_copy(side).wait_send()
        start_all(0, (side,))


    def step(side, k, t):
        new, middle, old = (halo_row(side, k - j) for j in range(3))
        span_rows(t, (new,), k == 1 or shifting and k == 2)
        filtered_rows(t, (middle,))
        stress_row(t, middle, k == 1)
        sums(t, (old,))

    for side in range(2):
        near_copy(1 - side).wait_recv()

        @pl.when(not_high)
        def _():
            c_copy(side, 1).start()

        @pl.when(not_low)
        def _():
            c_copy(side, 0).start()

    def near(i, carry):
        for side in range(2):
            step(side, 1, i)

        @pl.when(i == nt // 2)
        def _():
            start_all(1)

        return carry

    lax.fori_loop(1, nt + 1, near, 0)
    start_all(2)
    for side in range(2):
        start_moved(side)
    close_round(2)

    def later_round(k):
        open_round(k)
        close_round(k)

    for k in range(3, len(reaches)):
        later_round(k)
    to_ends(ring.at[len(reaches)])

    @pl.when(not_high)
    def _():
        c_all(0, 2, c_recv.at[0]).wait_recv()

    @pl.when(not_low)
    def _():
        c_all(1, 2, c_recv.at[1]).wait_recv()

    def corners(i, carry):
        t = i * (nt + 1)
        for side in range(2):
            span_rows(t, (halo_row(side, 1),), False)
            filtered_rows(t, (halo_row(side, 0),))
        return carry

    lax.fori_loop(0, 2, corners, 0)

    def far(p):
        def both(i, carry):
            for side in range(2):
                step(side, 2, order(i))
            return carry

        def one(side):
            def run(i, carry):
                step(side, 2, order(i))
                return carry

            return run

        if not shifting or p < pieces - 2:
            for side in range(2):
                wait_far(side, p)
            lax.fori_loop(cuts[p], cuts[p + 1], both, 0)
            return
        for side in range(2):
            @pl.when(gains[side] >= 0)
            def _():
                wait_far(side, p)
                lax.fori_loop(cuts[p], cuts[p + 1], one(side), 0)

    far(0)
    start_all(3)

    def column_sums(ref):
        ref[0:1, :] = jnp.sum(accn[...].T, axis=0, keepdims=True)
        ref[1:2, :] = jnp.sum(accd[...].T, axis=0, keepdims=True)

    def g_copy(kind, to_x, to_y):
        return pltpu.make_async_remote_copy(
            src_ref=mine if kind == 0 else mine_ends,
            dst_ref=gather.at[kind, gx],
            send_sem=g_send.at[kind],
            recv_sem=g_recv.at[kind],
            device_id=(to_x, to_y),
            device_id_type=MESH,
        )

    def g_all(kind):
        count = n - 1 if kind == 0 else n
        part = gather.at[kind, 0:count]
        return pltpu.make_async_remote_copy(
            src_ref=part,
            dst_ref=part,
            send_sem=g_send.at[kind],
            recv_sem=g_recv.at[kind],
            device_id=(right, gy),
            device_id_type=MESH,
        )

    column_sums(mine_ends)
    pl.semaphore_wait(ring.at[len(reaches)], ends)

    def send_ends(i, carry):
        @pl.when(not_low)
        def _():
            g_copy(2, i, gy - 1).start()

        @pl.when(not_high)
        def _():
            g_copy(1, i, gy + 1).start()

        return carry

    lax.fori_loop(0, n, send_ends, 0)

    for p in range(1, pieces):
        far(p)
        if p == 1:
            start_all(4)
    if shifting:
        for side in range(2):
            def run(i, carry):
                step(side, 3, i)
                return carry

            @pl.when(gains[side] > 0)
            def _():
                moved_copy(1 - side).wait_recv()
                lax.fori_loop(moved, nt, run, 0)

    column_sums(mine)

    def send(i, carry):
        @pl.when(i != gx)
        def _():
            g_copy(0, i, gy).start()

        return carry

    lax.fori_loop(0, n, send, 0)
    gather[0, gx] = mine[...]
    drain()

    @pl.when(not_low)
    def _():
        c_all(0, nx + 2, c_recv.at[0]).wait_send()

    @pl.when(not_high)
    def _():
        c_all(1, nx + 2, c_recv.at[1]).wait_send()

    @pl.when(not_low)
    def _():
        g_all(2).wait_send()

    @pl.when(not_high)
    def _():
        g_all(1).wait_send()

    @pl.when(not_low)
    def _():
        g_all(1).wait_recv()

    @pl.when(not_high)
    def _():
        g_all(2).wait_recv()

    def profile(kind):
        total = functools.reduce(lambda x, y: x + y, [gather[kind, i] for i in range(n)])
        return jnp.clip(2.0 * (total[0:1] / total[1:2]), 0.0, clip_high)

    low_raw = pltpu.roll(profile(1), (lanes + 1 - ny) % lanes, 1)
    high_raw = pltpu.roll(profile(2), ny - 1, 1)
    g_all(0).wait_recv()
    raw = profile(0)
    where = lax.broadcasted_iota(jnp.int32, (1, lanes), 1)
    first = where == 0
    last = where == ny - 1
    under = jnp.where(first, raw, pltpu.roll(raw, 1, 1))
    over = jnp.where(last, raw, pltpu.roll(raw, lanes - 1, 1))
    under = jnp.where(jnp.logical_and(first, not_low), low_raw, under)
    over = jnp.where(jnp.logical_and(last, not_high), high_raw, over)
    coef_ref[...] = 0.25 * under + 0.5 * raw + 0.25 * over
    g_all(0).wait_send()


def local(n, m, shifts, velocity):
    _, nx, ny, nz = velocity.shape
    lanes = -(-ny // 128) * 128
    nt = ny // 8
    f32 = jnp.float32
    strength, coef = pl.pallas_call(
        functools.partial(kernel, n, m, nx, ny, shifts),
        out_shape=(
            jax.ShapeDtypeStruct((nx, ny, nz), f32),
            jax.ShapeDtypeStruct((1, lanes), f32),
        ),
        in_specs=[pl.BlockSpec(memory_space=pltpu.HBM)],
        out_specs=(
            pl.BlockSpec(memory_space=pltpu.VMEM),
            pl.BlockSpec(memory_space=pltpu.VMEM),
        ),
        scratch_shapes=[
            pltpu.VMEM((3, nx + 2 * HALO, ny + 16, nz), f32),
            pltpu.VMEM((3, nx + 2 * HALO, ny + 16, nz), f32),
            pltpu.VMEM((3, nx + 2 * HALO, ny + 16, nz), f32),
            pltpu.VMEM((3, nx + 2 * HALO, ny + 16, nz), f32),
            pltpu.VMEM((6, nx + 2 * HALO, ny, nz), f32),
            pltpu.VMEM((lanes, 128), f32),
            pltpu.VMEM((lanes, 128), f32),
            pltpu.VMEM((2, lanes), f32),
            pltpu.VMEM((2, lanes), f32),
            pltpu.VMEM((3, n, 2, lanes), f32),
            pltpu.SemaphoreType.DMA((3,)),
            pltpu.SemaphoreType.DMA((2,)),
            pltpu.SemaphoreType.DMA((2, len(cuts_of(nt)) + (1 if any(shifts) else 0))),
            pltpu.SemaphoreType.DMA((2,)),
            pltpu.SemaphoreType.DMA((2,)),
            pltpu.SemaphoreType.DMA((2,)),
            pltpu.SemaphoreType.DMA((3,)),
            pltpu.SemaphoreType.DMA((3,)),
            pltpu.SemaphoreType.REGULAR((3,)),
            pltpu.SemaphoreType.REGULAR((n.bit_length() + 1,)),
        ],
        compiler_params=pltpu.CompilerParams(
            collective_id=0, has_side_effects=True, vmem_limit_bytes=32 * 1024 * 1024
        ),
    )(pltpu.with_memory_space_constraint(velocity, pltpu.HBM))
    smooth = coef[0, :ny]
    return (smooth, smooth[None, :, None] * strength)


def solution(mesh):
    n, m = mesh.shape["gx"], mesh.shape["gy"]
    shifts = (0,)*n
    return jax.shard_map(
        functools.partial(local, n, m, shifts),
        mesh=mesh,
        in_specs=(P(None, "gx", "gy", None),),
        out_specs=(P("gy"), P("gx", "gy", None)),
        check_vma=False,
    )
```

```python
import functools

import jax
import jax.numpy as jnp
from jax import lax
from jax.experimental import pallas as pl
from jax.experimental.pallas import tpu as pltpu
from jax.sharding import PartitionSpec as P

clip_high = 0.1
pairs = ((0, 0), (1, 1), (2, 2), (0, 1), (0, 2), (1, 2))
MESH = pl.DeviceIdType.MESH
HALO = 3


def tile(index):
    return pl.ds(pl.multiple_of(index * 8, 8), 8)


def roll_next(value):
    return pltpu.roll(value, value.shape[1] - 1, 1)


def roll_prev(value):
    return pltpu.roll(value, 1, 1)


def filter_span(value):
    return (roll_next(value) + roll_prev(value)) + 2.0 * value


def slope_span(value):
    return roll_next(value) - roll_prev(value)


def slope_wall(ref, comp, row, t, here):
    rows = lax.broadcasted_iota(jnp.int32, here.shape, 0)
    below = ref[comp, row, tile(t - 1), :]
    above = ref[comp, row, tile(t + 1), :]
    up = pltpu.roll(jnp.where(rows == 0, above, here), 7, 0)
    down = pltpu.roll(jnp.where(rows == 7, below, here), 1, 0)
    return up - down


def strain4(ref, row, t, slope=None):
    here = [ref[c, row, tile(t), :] for c in range(3)]
    dx = [ref[c, row + 1, tile(t), :] - ref[c, row - 1, tile(t), :] for c in range(3)]
    dy = [slope_wall(ref, c, row, t, here[c]) for c in range(3)]
    if slope is None:
        dz = [slope_span(here[c]) for c in range(3)]
    else:
        dz = [slope[c, row, tile(t), :] for c in range(3)]
    s = (
        dx[0],
        4.0 * dy[1],
        2.0 * dz[2],
        2.0 * dy[0] + 0.5 * dx[1],
        dz[0] + 0.5 * dx[2],
        dz[1] + 2.0 * dy[2],
    )
    diag = s[0] * s[0] + s[1] * s[1] + s[2] * s[2]
    off = s[3] * s[3] + s[4] * s[4] + s[5] * s[5]
    return here, s, diag + 2.0 * off


def cuts_of(nt):
    edges = [0, min(3, nt)]
    while nt - edges[-1] > 1:
        edges.append(min(edges[-1] + 2, nt - 1))
    if edges[-1] < nt:
        edges.append(nt)
    return edges


def kernel(n, m, nx, ny, shifts, u_hbm, strength, coef_ref, u, w, v, d, g, accn, accd,
           mine, mine_ends, gather, own_sem, xs_send, xs_recv, y_send, y_recv,
           c_recv, g_send, g_recv, ready, ring):
    nt = ny // 8
    edge_lo, edge_hi = HALO, HALO + nx - 1
    gx = lax.axis_index("gx")
    gy = lax.axis_index("gy")
    left, right = lax.rem(gx + n - 1, n), lax.rem(gx + 1, n)
    not_low, not_high = gy > 0, gy < m - 1
    begins, closes = gx == 0, gx == n - 1
    lanes = mine.shape[-1]
    shifting = any(shifts)
    cuts = cuts_of(nt)
    pieces = len(cuts) - 1
    moved = cuts[max(pieces - 2, 1)]

    def shift_at(index):
        value = jnp.int32(shifts[0])
        for i in range(1, n):
            if shifts[i] != shifts[0]:
                value = jnp.where(index == i, jnp.int32(shifts[i]), value)
        return value

    gains = (shift_at(left), -shift_at(gx)) if shifting else (0, 0)

    own = [
        pltpu.make_async_copy(
            u_hbm.at[:, a:b, :, :], u.at[:, edge_lo + a:edge_lo + b, 8:8 + ny, :], own_sem.at[k]
        )
        for k, (a, b) in enumerate(((0, 1), (nx - 1, nx), (1, nx - 1)))
    ]
    for copy in own:
        copy.start()

    def signal(semaphore, to_x, to_y):
        pl.semaphore_signal(semaphore, inc=1, device_id=(to_x, to_y), device_id_type=MESH)

    barrier = pltpu.get_barrier_semaphore()

    even = lax.rem(gx, 2) == 0
    paired = jnp.logical_or(jnp.logical_not(even), gx < n - 1)
    waits_right = jnp.logical_and(jnp.logical_not(even), jnp.logical_not(closes))
    later_left = jnp.logical_and(even, gx > 0)

    @pl.when(paired)
    def _():
        signal(barrier, jnp.where(even, right, left), gy)

    @pl.when(waits_right)
    def _():
        signal(barrier, right, gy)

    @pl.when(begins)
    def _():
        signal(barrier, left, gy)

    @pl.when(not_high)
    def _():
        signal(barrier, gx, gy + 1)

    earlier = [jnp.where(x, 1, 0) for x in (paired, later_left, closes, not_low)]
    greeted = sum(earlier)

    @pl.when(greeted > 0)
    def _():
        pl.semaphore_wait(barrier, greeted)

    @pl.when(later_left)
    def _():
        signal(ready.at[0], left, gy)

    @pl.when(closes)
    def _():
        signal(ready.at[1], right, gy)

    @pl.when(not_low)
    def _():
        signal(ready.at[2], gx, gy - 1)

    ends = jnp.where(not_low, 1, 0) + jnp.where(not_high, 1, 0)
    reaches = [2 ** k for k in range(n.bit_length()) if 2 ** k < n]

    def open_round(k):
        if k < len(reaches):
            @pl.when(gx >= reaches[k])
            def _():
                signal(ring.at[k], gx - reaches[k], gy)

            @pl.when(gx < n - reaches[k])
            def _():
                signal(ring.at[k], gx + reaches[k], gy)

    def close_round(k):
        if k < len(reaches):
            near = (gx >= reaches[k], gx < n - reaches[k])
            count = jnp.where(near[0], 1, 0) + jnp.where(near[1], 1, 0)

            @pl.when(count > 0)
            def _():
                pl.semaphore_wait(ring.at[k], count)

    def to_ends(semaphore):
        @pl.when(not_low)
        def _():
            signal(semaphore, gx, gy - 1)

        @pl.when(not_high)
        def _():
            signal(semaphore, gx, gy + 1)

    def order(i):
        return jnp.where(i == 0, nt, i)

    def halo_row(side, k):
        return edge_lo - k if side == 0 else edge_hi + k

    def x_copy(side, k, low, high, slot):
        src = halo_row(side, 1 - k)
        dst = halo_row(1 - side, k)
        return pltpu.make_async_remote_copy(
            src_ref=u.at[:, src:src + 1, 8 * low:8 * high, :],
            dst_ref=u.at[:, dst:dst + 1, 8 * low:8 * high, :],
            send_sem=xs_send.at[side],
            recv_sem=xs_recv.at[1 - side, slot],
            device_id=(left if side == 0 else right, gy),
            device_id_type=MESH,
        )

    def near_copy(side):
        return x_copy(side, 1, 1, nt + 1, 0)

    def moved_copy(side):
        return x_copy(side, 3, moved, nt, pieces + 1)

    def far_parts(p):
        if p == 0:
            return [(nt, nt + 1), (1, cuts[1])] if cuts[1] > 1 else [(nt, nt + 1)]
        return [(cuts[p], cuts[p + 1])]

    def start_far(side, p):
        def run():
            for low, high in far_parts(p):
                x_copy(side, 2, low, high, p + 1).start()

        if shifting and p >= pieces - 2:
            pl.when(gains[side] <= 0)(run)
        else:
            run()

    def start_moved(side):
        if shifting:
            @pl.when(gains[side] < 0)
            def _():
                moved_copy(side).start()

    def wait_far(side, p):
        count = cuts[p + 1] - cuts[p]
        x_copy(1 - side, 2, 1, 1 + count, p + 1).wait_recv()

    def tiles_view(count):
        rows = next(r for r in range(1, u.shape[1] + 1) if count % r == 0 and count // r <= nt + 2)
        return u.at[:, 0:rows, 0:8 * (count // rows), :]

    def drain():
        for side in range(2):
            if not shifting:
                wait_rows(side, tiles_view(nt))
                continue
            for sign, count in ((0, nt), (1, moved), (-1, 2 * nt - moved)):
                @pl.when(gains[side] == sign)
                def _():
                    wait_rows(side, tiles_view(count))

    def y_copy(side):
        src = 8 if side == 0 else ny + 7
        dst = ny + 8 if side == 0 else 7
        return pltpu.make_async_remote_copy(
            src_ref=u.at[:, edge_lo:edge_lo + nx, src:src + 1, :],
            dst_ref=u.at[:, edge_lo:edge_lo + nx, dst:dst + 1, :],
            send_sem=y_send.at[side],
            recv_sem=y_recv.at[side],
            device_id=(gx, gy - 1 if side == 0 else gy + 1),
            device_id_type=MESH,
        )

    def c_copy(side, end):
        row = halo_row(side, 1)
        src = 8 if end == 0 else ny + 7
        dst = ny + 8 if end == 0 else 7
        return pltpu.make_async_remote_copy(
            src_ref=u.at[:, row:row + 1, src:src + 1, :],
            dst_ref=u.at[:, row:row + 1, dst:dst + 1, :],
            send_sem=y_send.at[end],
            recv_sem=c_recv.at[end],
            device_id=(gx, gy - 1 if end == 0 else gy + 1),
            device_id_type=MESH,
        )

    def c_all(end, rows, semaphore):
        part = u.at[:, 0:rows, 8:9, :]
        return pltpu.make_async_remote_copy(
            src_ref=part,
            dst_ref=part,
            send_sem=y_send.at[end],
            recv_sem=semaphore,
            device_id=(gx, gy - 1 if end == 0 else gy + 1),
            device_id_type=MESH,
        )

    def wait_rows(side, part):
        pltpu.make_async_remote_copy(
            src_ref=part,
            dst_ref=part,
            send_sem=xs_send.at[side],
            recv_sem=xs_recv.at[1 - side, 0],
            device_id=(left if side == 0 else right, gy),
            device_id_type=MESH,
        ).wait_send()

    plans = (((0, 1), (2, 3), (), (), ()), ((0,), (), (1, 2, 3), (), ()))
    odd = lax.rem(gy, 2) == 1

    def start_all(point, sides=(0, 1)):
        chosen = [[p for p in plan[point] if p < pieces] for plan in plans]

        def run(parts):
            for p in parts:
                for side in sides:
                    start_far(side, p)

        if chosen[0] == chosen[1]:
            run(chosen[0])
            return
        if chosen[0]:
            pl.when(jnp.logical_not(odd))(lambda: run(chosen[0]))
        if chosen[1]:
            pl.when(odd)(lambda: run(chosen[1]))

    own[0].wait()

    @pl.when(gx > 0)
    def _():
        near_copy(0).start()

    own[1].wait()

    @pl.when(jnp.logical_not(waits_right))
    def _():
        near_copy(1).start()

    own[2].wait()

    @pl.when(not_low)
    def _():
        y_copy(0).start()

    @pl.when(waits_right)
    def _():
        pl.semaphore_wait(ready.at[0], 1)
        near_copy(1).start()

    open_round(0)

    @pl.when(not_high)
    def _():
        pl.semaphore_wait(ready.at[2], 1)
        y_copy(1).start()

    accn[...] = jnp.zeros_like(accn)
    accd[...] = jnp.zeros_like(accd)
    rows_all = u.shape[1]

    @pl.when(jnp.logical_not(not_low))
    def _():
        u[:, :, 0:8, :] = jnp.zeros((3, rows_all, 8, u.shape[3]), jnp.float32)

    @pl.when(jnp.logical_not(not_high))
    def _():
        u[:, :, ny + 8:ny + 16, :] = jnp.zeros((3, rows_all, 8, u.shape[3]), jnp.float32)

    def span_rows(t, rows, slopes=True):
        for c in range(3):
            for row in rows:
                here = u[c, row, tile(t), :]
                after, before = roll_next(here), roll_prev(here)
                w[c, row, tile(t), :] = (after + before) + 2.0 * here
                if slopes:
                    d[c, row, tile(t), :] = after - before

    def filtered_rows(t, rows):
        for c in range(3):
            for row in rows:
                a, b, e = (w[c, row + k, tile(t), :] for k in (-1, 0, 1))
                v[c, row, tile(t), :] = 0.25 * ((a + e) + 2.0 * b)

    def stress_row(t, row, keep):
        _, s, total = strain4(u, row, t, d)
        size = jnp.sqrt(0.125 * total)
        if keep:
            strength[row - edge_lo, tile(t - 1), :] = size
        for k in range(6):
            g[k, row, tile(t - 1), :] = size * s[k]

    def sums_row(t, row):
        centre, s, total = strain4(v, row, t)
        scale = jnp.sqrt(2.0 * total)

        def product(a, b):
            one, two, three = (near[j][a] * near[j][b] for j in range(3))
            return filter_span((one + three) + 2.0 * two)

        def stress(k):
            one, two, three = (g[k, row + j, tile(t - 1), :] for j in (-1, 0, 1))
            return filter_span((one + three) + 2.0 * two)

        near = [[u[c, row + j, tile(t), :] for c in range(3)] for j in (-1, 0, 1)]
        leonard = [product(a, b) - centre[a] * centre[b] for a, b in pairs]
        third = (leonard[0] + leonard[1] + leonard[2]) * (1.0 / 3.0)
        leonard = [x - third for x in leonard[:3]] + leonard[3:]
        model = [stress(k) - scale * s[k] for k in range(6)]
        lm = [x * y for x, y in zip(leonard, model)]
        mm = [x * x for x in model]
        num = (lm[0] + lm[1] + lm[2]) + 2.0 * (lm[3] + lm[4] + lm[5])
        den = (mm[0] + mm[1] + mm[2]) + 2.0 * (mm[3] + mm[4] + mm[5])
        return num, den

    def fold(value):
        parts = [value[:, k:k + 128] for k in range(0, value.shape[1], 128)]
        return functools.reduce(lambda x, y: x + y, parts)

    def sums(t, rows):
        both = [sums_row(t, row) for row in rows]
        num = functools.reduce(lambda x, y: x + y, [b[0] for b in both])
        den = functools.reduce(lambda x, y: x + y, [b[1] for b in both])
        accn[tile(t - 1), :] += fold(num)
        accd[tile(t - 1), :] += fold(den)

    def inner_filter(t, carry):
        span_rows(t, range(edge_lo, edge_hi + 1))
        filtered_rows(t, range(edge_lo + 1, edge_hi))
        return carry

    lax.fori_loop(1, nt + 1, inner_filter, 0)

    @pl.when(not_high)
    def _():
        y_copy(0).wait_recv()

    @pl.when(not_low)
    def _():
        y_copy(1).wait_recv()

    def end_filter(i, carry):
        return inner_filter(i * (nt + 1), carry)

    lax.fori_loop(0, 2, end_filter, 0)

    half = (nx - 2) // 2

    def inner_stress(i, carry):
        t = i // half + 1
        row = edge_lo + 1 + 2 * lax.rem(i, half)
        stress_row(t, row, True)
        stress_row(t, row + 1, True)
        return carry

    lax.fori_loop(0, nt * half, inner_stress, 0)
    close_round(0)
    open_round(1)

    @pl.when(begins)
    def _():
        pl.semaphore_wait(ready.at[1], 1)
        near_copy(0).start()

    def inner_sums(t, carry):
        sums(t, range(edge_lo + 2, edge_hi - 1))
        return carry

    lax.fori_loop(1, nt + 1, inner_sums, 0)
    close_round(1)
    open_round(2)

    for side in range(2):
        near_copy(side).wait_send()
        start_all(0, (side,))


    def step(side, k, t):
        new, middle, old = (halo_row(side, k - j) for j in range(3))
        span_rows(t, (new,), k == 1 or shifting and k == 2)
        filtered_rows(t, (middle,))
        stress_row(t, middle, k == 1)
        sums(t, (old,))

    for side in range(2):
        near_copy(1 - side).wait_recv()

        @pl.when(not_high)
        def _():
            c_copy(side, 1).start()

        @pl.when(not_low)
        def _():
            c_copy(side, 0).start()

    def near(i, carry):
        for side in range(2):
            step(side, 1, i)

        @pl.when(i == nt // 2)
        def _():
            start_all(1)

        return carry

    lax.fori_loop(1, nt + 1, near, 0)
    start_all(2)
    for side in range(2):
        start_moved(side)
    close_round(2)

    def later_round(k):
        open_round(k)
        close_round(k)

    for k in range(3, len(reaches)):
        later_round(k)
    to_ends(ring.at[len(reaches)])

    @pl.when(not_high)
    def _():
        c_all(0, 2, c_recv.at[0]).wait_recv()

    @pl.when(not_low)
    def _():
        c_all(1, 2, c_recv.at[1]).wait_recv()

    def corners(i, carry):
        t = i * (nt + 1)
        for side in range(2):
            span_rows(t, (halo_row(side, 1),), False)
            filtered_rows(t, (halo_row(side, 0),))
        return carry

    lax.fori_loop(0, 2, corners, 0)

    def far(p):
        def both(i, carry):
            for side in range(2):
                step(side, 2, order(i))
            return carry

        def one(side):
            def run(i, carry):
                step(side, 2, order(i))
                return carry

            return run

        if not shifting or p < pieces - 2:
            for side in range(2):
                wait_far(side, p)
            lax.fori_loop(cuts[p], cuts[p + 1], both, 0)
            return
        for side in range(2):
            @pl.when(gains[side] >= 0)
            def _():
                wait_far(side, p)
                lax.fori_loop(cuts[p], cuts[p + 1], one(side), 0)

    far(0)
    start_all(3)

    def column_sums(ref):
        ref[0:1, :] = jnp.sum(accn[...].T, axis=0, keepdims=True)
        ref[1:2, :] = jnp.sum(accd[...].T, axis=0, keepdims=True)

    def g_copy(kind, to_x, to_y):
        return pltpu.make_async_remote_copy(
            src_ref=mine if kind == 0 else mine_ends,
            dst_ref=gather.at[kind, gx],
            send_sem=g_send.at[kind],
            recv_sem=g_recv.at[kind],
            device_id=(to_x, to_y),
            device_id_type=MESH,
        )

    def g_all(kind):
        count = n - 1 if kind == 0 else n
        part = gather.at[kind, 0:count]
        return pltpu.make_async_remote_copy(
            src_ref=part,
            dst_ref=part,
            send_sem=g_send.at[kind],
            recv_sem=g_recv.at[kind],
            device_id=(right, gy),
            device_id_type=MESH,
        )

    column_sums(mine_ends)
    pl.semaphore_wait(ring.at[len(reaches)], ends)

    def send_ends(i, carry):
        @pl.when(not_low)
        def _():
            g_copy(2, i, gy - 1).start()

        @pl.when(not_high)
        def _():
            g_copy(1, i, gy + 1).start()

        return carry

    lax.fori_loop(0, n, send_ends, 0)

    for p in range(1, pieces):
        far(p)
        if p == 1:
            start_all(4)
    if shifting:
        for side in range(2):
            def run(i, carry):
                step(side, 3, i)
                return carry

            @pl.when(gains[side] > 0)
            def _():
                moved_copy(1 - side).wait_recv()
                lax.fori_loop(moved, nt, run, 0)

    column_sums(mine)

    def send(i, carry):
        @pl.when(i != gx)
        def _():
            g_copy(0, i, gy).start()

        return carry

    lax.fori_loop(0, n, send, 0)
    gather[0, gx] = mine[...]
    drain()

    @pl.when(not_low)
    def _():
        c_all(0, nx + 2, c_recv.at[0]).wait_send()

    @pl.when(not_high)
    def _():
        c_all(1, nx + 2, c_recv.at[1]).wait_send()

    @pl.when(not_low)
    def _():
        g_all(2).wait_send()

    @pl.when(not_high)
    def _():
        g_all(1).wait_send()

    @pl.when(not_low)
    def _():
        g_all(1).wait_recv()

    @pl.when(not_high)
    def _():
        g_all(2).wait_recv()

    def profile(kind):
        total = functools.reduce(lambda x, y: x + y, [gather[kind, i] for i in range(n)])
        return jnp.clip(2.0 * (total[0:1] / total[1:2]), 0.0, clip_high)

    low_raw = pltpu.roll(profile(1), (lanes + 1 - ny) % lanes, 1)
    high_raw = pltpu.roll(profile(2), ny - 1, 1)
    g_all(0).wait_recv()
    raw = profile(0)
    where = lax.broadcasted_iota(jnp.int32, (1, lanes), 1)
    first = where == 0
    last = where == ny - 1
    under = jnp.where(first, raw, pltpu.roll(raw, 1, 1))
    over = jnp.where(last, raw, pltpu.roll(raw, lanes - 1, 1))
    under = jnp.where(jnp.logical_and(first, not_low), low_raw, under)
    over = jnp.where(jnp.logical_and(last, not_high), high_raw, over)
    coef_ref[...] = 0.25 * under + 0.5 * raw + 0.25 * over
    g_all(0).wait_send()


def local(n, m, shifts, velocity):
    _, nx, ny, nz = velocity.shape
    lanes = -(-ny // 128) * 128
    nt = ny // 8
    f32 = jnp.float32
    strength, coef = pl.pallas_call(
        functools.partial(kernel, n, m, nx, ny, shifts),
        out_shape=(
            jax.ShapeDtypeStruct((nx, ny, nz), f32),
            jax.ShapeDtypeStruct((1, lanes), f32),
        ),
        in_specs=[pl.BlockSpec(memory_space=pltpu.HBM)],
        out_specs=(
            pl.BlockSpec(memory_space=pltpu.VMEM),
            pl.BlockSpec(memory_space=pltpu.VMEM),
        ),
        scratch_shapes=[
            pltpu.VMEM((3, nx + 2 * HALO, ny + 16, nz), f32),
            pltpu.VMEM((3, nx + 2 * HALO, ny + 16, nz), f32),
            pltpu.VMEM((3, nx + 2 * HALO, ny + 16, nz), f32),
            pltpu.VMEM((3, nx + 2 * HALO, ny + 16, nz), f32),
            pltpu.VMEM((6, nx + 2 * HALO, ny, nz), f32),
            pltpu.VMEM((lanes, 128), f32),
            pltpu.VMEM((lanes, 128), f32),
            pltpu.VMEM((2, lanes), f32),
            pltpu.VMEM((2, lanes), f32),
            pltpu.VMEM((3, n, 2, lanes), f32),
            pltpu.SemaphoreType.DMA((3,)),
            pltpu.SemaphoreType.DMA((2,)),
            pltpu.SemaphoreType.DMA((2, len(cuts_of(nt)) + (1 if any(shifts) else 0))),
            pltpu.SemaphoreType.DMA((2,)),
            pltpu.SemaphoreType.DMA((2,)),
            pltpu.SemaphoreType.DMA((2,)),
            pltpu.SemaphoreType.DMA((3,)),
            pltpu.SemaphoreType.DMA((3,)),
            pltpu.SemaphoreType.REGULAR((3,)),
            pltpu.SemaphoreType.REGULAR((n.bit_length() + 1,)),
        ],
        compiler_params=pltpu.CompilerParams(
            collective_id=0, has_side_effects=True, vmem_limit_bytes=32 * 1024 * 1024
        ),
    )(pltpu.with_memory_space_constraint(velocity, pltpu.HBM))
    smooth = coef[0, :ny]
    return (smooth, smooth[None, :, None] * strength)


def solution(mesh):
    n, m = mesh.shape["gx"], mesh.shape["gy"]
    shifts = (0,)*n
    return jax.shard_map(
        functools.partial(local, n, m, shifts),
        mesh=mesh,
        in_specs=(P(None, "gx", "gy", None),),
        out_specs=(P("gy"), P("gx", "gy", None)),
        check_vma=False,
    )
```

```python
import functools

import jax
import jax.numpy as jnp
from jax import lax
from jax.experimental import pallas as pl
from jax.experimental.pallas import tpu as pltpu
from jax.sharding import PartitionSpec as P

clip_high = 0.1
pairs = ((0, 0), (1, 1), (2, 2), (0, 1), (0, 2), (1, 2))
MESH = pl.DeviceIdType.MESH
HALO = 3


def tile(index):
    return pl.ds(pl.multiple_of(index * 8, 8), 8)


def roll_next(value):
    return pltpu.roll(value, value.shape[1] - 1, 1)


def roll_prev(value):
    return pltpu.roll(value, 1, 1)


def filter_span(value):
    return (roll_next(value) + roll_prev(value)) + 2.0 * value


def slope_span(value):
    return roll_next(value) - roll_prev(value)


def slope_wall(ref, comp, row, t, here):
    rows = lax.broadcasted_iota(jnp.int32, here.shape, 0)
    below = ref[comp, row, tile(t - 1), :]
    above = ref[comp, row, tile(t + 1), :]
    up = pltpu.roll(jnp.where(rows == 0, above, here), 7, 0)
    down = pltpu.roll(jnp.where(rows == 7, below, here), 1, 0)
    return up - down


def strain4(ref, row, t, slope=None):
    here = [ref[c, row, tile(t), :] for c in range(3)]
    dx = [ref[c, row + 1, tile(t), :] - ref[c, row - 1, tile(t), :] for c in range(3)]
    dy = [slope_wall(ref, c, row, t, here[c]) for c in range(3)]
    if slope is None:
        dz = [slope_span(here[c]) for c in range(3)]
    else:
        dz = [slope[c, row, tile(t), :] for c in range(3)]
    s = (
        dx[0],
        4.0 * dy[1],
        2.0 * dz[2],
        2.0 * dy[0] + 0.5 * dx[1],
        dz[0] + 0.5 * dx[2],
        dz[1] + 2.0 * dy[2],
    )
    diag = s[0] * s[0] + s[1] * s[1] + s[2] * s[2]
    off = s[3] * s[3] + s[4] * s[4] + s[5] * s[5]
    return here, s, diag + 2.0 * off


def cuts_of(nt):
    edges = [0, min(3, nt)]
    while nt - edges[-1] > 1:
        edges.append(min(edges[-1] + 2, nt - 1))
    if edges[-1] < nt:
        edges.append(nt)
    return edges


def amounts_of(shifts):
    return sorted({abs(s) for s in shifts} - {0})


def kernel(n, m, nx, ny, shifts, u_hbm, strength, coef_ref, u, w, v, d, g, accn, accd,
           mine, mine_ends, gather, own_sem, xs_send, xs_recv, y_send, y_recv,
           c_recv, g_send, g_recv, ready, ring):
    nt = ny // 8
    edge_lo, edge_hi = HALO, HALO + nx - 1
    gx = lax.axis_index("gx")
    gy = lax.axis_index("gy")
    left, right = lax.rem(gx + n - 1, n), lax.rem(gx + 1, n)
    not_low, not_high = gy > 0, gy < m - 1
    begins, closes = gx == 0, gx == n - 1
    lanes = mine.shape[-1]
    shifting = any(shifts)
    cuts = cuts_of(nt)
    pieces = len(cuts) - 1
    amounts = amounts_of(shifts)

    def shift_at(index):
        value = jnp.int32(shifts[0])
        for i in range(1, n):
            if shifts[i] != shifts[0]:
                value = jnp.where(index == i, jnp.int32(shifts[i]), value)
        return value

    gains = (shift_at(left), -shift_at(gx)) if shifting else (0, 0)

    own = [
        pltpu.make_async_copy(
            u_hbm.at[:, a:b, :, :], u.at[:, edge_lo + a:edge_lo + b, 8:8 + ny, :], own_sem.at[k]
        )
        for k, (a, b) in enumerate(((0, 1), (nx - 1, nx), (1, nx - 1)))
    ]
    for copy in own:
        copy.start()

    def signal(semaphore, to_x, to_y):
        pl.semaphore_signal(semaphore, inc=1, device_id=(to_x, to_y), device_id_type=MESH)

    barrier = pltpu.get_barrier_semaphore()

    even = lax.rem(gx, 2) == 0
    paired = jnp.logical_or(jnp.logical_not(even), gx < n - 1)
    waits_right = jnp.logical_and(jnp.logical_not(even), jnp.logical_not(closes))
    later_left = jnp.logical_and(even, gx > 0)

    @pl.when(paired)
    def _():
        signal(barrier, jnp.where(even, right, left), gy)

    @pl.when(waits_right)
    def _():
        signal(barrier, right, gy)

    @pl.when(begins)
    def _():
        signal(barrier, left, gy)

    @pl.when(not_high)
    def _():
        signal(barrier, gx, gy + 1)

    earlier = [jnp.where(x, 1, 0) for x in (paired, later_left, closes, not_low)]
    greeted = sum(earlier)

    @pl.when(greeted > 0)
    def _():
        pl.semaphore_wait(barrier, greeted)

    @pl.when(later_left)
    def _():
        signal(ready.at[0], left, gy)

    @pl.when(closes)
    def _():
        signal(ready.at[1], right, gy)

    @pl.when(not_low)
    def _():
        signal(ready.at[2], gx, gy - 1)

    ends = jnp.where(not_low, 1, 0) + jnp.where(not_high, 1, 0)
    reaches = [2 ** k for k in range(n.bit_length()) if 2 ** k < n]

    def open_round(k):
        if k < len(reaches):
            @pl.when(gx >= reaches[k])
            def _():
                signal(ring.at[k], gx - reaches[k], gy)

            @pl.when(gx < n - reaches[k])
            def _():
                signal(ring.at[k], gx + reaches[k], gy)

    def close_round(k):
        if k < len(reaches):
            near = (gx >= reaches[k], gx < n - reaches[k])
            count = jnp.where(near[0], 1, 0) + jnp.where(near[1], 1, 0)

            @pl.when(count > 0)
            def _():
                pl.semaphore_wait(ring.at[k], count)

    def to_ends(semaphore):
        @pl.when(not_low)
        def _():
            signal(semaphore, gx, gy - 1)

        @pl.when(not_high)
        def _():
            signal(semaphore, gx, gy + 1)

    def order(i):
        return jnp.where(i == 0, nt, i)

    def halo_row(side, k):
        return edge_lo - k if side == 0 else edge_hi + k

    def x_copy(side, k, low, high, slot):
        src = halo_row(side, 1 - k)
        dst = halo_row(1 - side, k)
        return pltpu.make_async_remote_copy(
            src_ref=u.at[:, src:src + 1, 8 * low:8 * high, :],
            dst_ref=u.at[:, dst:dst + 1, 8 * low:8 * high, :],
            send_sem=xs_send.at[side],
            recv_sem=xs_recv.at[1 - side, slot],
            device_id=(left if side == 0 else right, gy),
            device_id_type=MESH,
        )

    def near_copy(side):
        return x_copy(side, 1, 1, nt + 1, 0)

    def moved_tiles(j):
        high = pieces - amounts[j - 1] if j else pieces
        return cuts[pieces - amounts[j]], cuts[high]

    def moved_copy(side, j):
        return x_copy(side, 3, *moved_tiles(j), pieces + 1 + j)

    def far_parts(p):
        if p == 0:
            return [(nt, nt + 1), (1, cuts[1])] if cuts[1] > 1 else [(nt, nt + 1)]
        return [(cuts[p], cuts[p + 1])]

    def start_far(side, p):
        def run():
            for low, high in far_parts(p):
                x_copy(side, 2, low, high, p + 1).start()

        if shifting and p >= pieces - amounts[-1]:
            pl.when(p < pieces - gains[side])(run)
        else:
            run()

    def start_moved(side):
        for j in range(len(amounts)):
            @pl.when(gains[side] <= -amounts[j])
            def _():
                moved_copy(side, j).start()

    def wait_far(side, p):
        count = cuts[p + 1] - cuts[p]
        x_copy(1 - side, 2, 1, 1 + count, p + 1).wait_recv()

    def tiles_view(count):
        rows = next(r for r in range(1, u.shape[1] + 1) if count % r == 0 and count // r <= nt + 2)
        return u.at[:, 0:rows, 0:8 * (count // rows), :]

    def drain():
        for side in range(2):
            if not shifting:
                wait_rows(side, tiles_view(nt))
                continue
            kept = [cuts[pieces - a] for a in amounts]
            cases = [(0, nt)] + list(zip(amounts, kept)) + [(-a, 2 * nt - c) for a, c in zip(amounts, kept)]
            for gain, count in cases:
                @pl.when(gains[side] == gain)
                def _():
                    wait_rows(side, tiles_view(count))

    def y_copy(side):
        src = 8 if side == 0 else ny + 7
        dst = ny + 8 if side == 0 else 7
        return pltpu.make_async_remote_copy(
            src_ref=u.at[:, edge_lo:edge_lo + nx, src:src + 1, :],
            dst_ref=u.at[:, edge_lo:edge_lo + nx, dst:dst + 1, :],
            send_sem=y_send.at[side],
            recv_sem=y_recv.at[side],
            device_id=(gx, gy - 1 if side == 0 else gy + 1),
            device_id_type=MESH,
        )

    def c_copy(side, end):
        row = halo_row(side, 1)
        src = 8 if end == 0 else ny + 7
        dst = ny + 8 if end == 0 else 7
        return pltpu.make_async_remote_copy(
            src_ref=u.at[:, row:row + 1, src:src + 1, :],
            dst_ref=u.at[:, row:row + 1, dst:dst + 1, :],
            send_sem=y_send.at[end],
            recv_sem=c_recv.at[end],
            device_id=(gx, gy - 1 if end == 0 else gy + 1),
            device_id_type=MESH,
        )

    def c_all(end, rows, semaphore):
        part = u.at[:, 0:rows, 8:9, :]
        return pltpu.make_async_remote_copy(
            src_ref=part,
            dst_ref=part,
            send_sem=y_send.at[end],
            recv_sem=semaphore,
            device_id=(gx, gy - 1 if end == 0 else gy + 1),
            device_id_type=MESH,
        )

    def wait_rows(side, part):
        pltpu.make_async_remote_copy(
            src_ref=part,
            dst_ref=part,
            send_sem=xs_send.at[side],
            recv_sem=xs_recv.at[1 - side, 0],
            device_id=(left if side == 0 else right, gy),
            device_id_type=MESH,
        ).wait_send()

    plans = (((0, 1), (2, 3), (), (), ()), ((0,), (), (1, 2, 3), (), ()))
    odd = lax.rem(gy, 2) == 1

    def start_all(point, sides=(0, 1)):
        chosen = [[p for p in plan[point] if p < pieces] for plan in plans]

        def run(parts):
            for p in parts:
                for side in sides:
                    start_far(side, p)

        if chosen[0] == chosen[1]:
            run(chosen[0])
            return
        if chosen[0]:
            pl.when(jnp.logical_not(odd))(lambda: run(chosen[0]))
        if chosen[1]:
            pl.when(odd)(lambda: run(chosen[1]))

    own[0].wait()

    @pl.when(gx > 0)
    def _():
        near_copy(0).start()

    own[1].wait()

    @pl.when(jnp.logical_not(waits_right))
    def _():
        near_copy(1).start()

    own[2].wait()

    @pl.when(not_low)
    def _():
        y_copy(0).start()

    @pl.when(waits_right)
    def _():
        pl.semaphore_wait(ready.at[0], 1)
        near_copy(1).start()

    open_round(0)

    @pl.when(not_high)
    def _():
        pl.semaphore_wait(ready.at[2], 1)
        y_copy(1).start()

    accn[...] = jnp.zeros_like(accn)
    accd[...] = jnp.zeros_like(accd)
    rows_all = u.shape[1]

    @pl.when(jnp.logical_not(not_low))
    def _():
        u[:, :, 0:8, :] = jnp.zeros((3, rows_all, 8, u.shape[3]), jnp.float32)

    @pl.when(jnp.logical_not(not_high))
    def _():
        u[:, :, ny + 8:ny + 16, :] = jnp.zeros((3, rows_all, 8, u.shape[3]), jnp.float32)

    def span_rows(t, rows, slopes=True):
        for c in range(3):
            for row in rows:
                here = u[c, row, tile(t), :]
                after, before = roll_next(here), roll_prev(here)
                w[c, row, tile(t), :] = (after + before) + 2.0 * here
                if slopes:
                    d[c, row, tile(t), :] = after - before

    def filtered_rows(t, rows):
        for c in range(3):
            for row in rows:
                a, b, e = (w[c, row + k, tile(t), :] for k in (-1, 0, 1))
                v[c, row, tile(t), :] = 0.25 * ((a + e) + 2.0 * b)

    def stress_row(t, row, keep):
        _, s, total = strain4(u, row, t, d)
        size = jnp.sqrt(0.125 * total)
        if keep:
            strength[row - edge_lo, tile(t - 1), :] = size
        for k in range(6):
            g[k, row, tile(t - 1), :] = size * s[k]

    def sums_row(t, row):
        centre, s, total = strain4(v, row, t)
        scale = jnp.sqrt(2.0 * total)

        def product(a, b):
            one, two, three = (near[j][a] * near[j][b] for j in range(3))
            return filter_span((one + three) + 2.0 * two)

        def stress(k):
            one, two, three = (g[k, row + j, tile(t - 1), :] for j in (-1, 0, 1))
            return filter_span((one + three) + 2.0 * two)

        near = [[u[c, row + j, tile(t), :] for c in range(3)] for j in (-1, 0, 1)]
        leonard = [product(a, b) - centre[a] * centre[b] for a, b in pairs]
        third = (leonard[0] + leonard[1] + leonard[2]) * (1.0 / 3.0)
        leonard = [x - third for x in leonard[:3]] + leonard[3:]
        model = [stress(k) - scale * s[k] for k in range(6)]
        lm = [x * y for x, y in zip(leonard, model)]
        mm = [x * x for x in model]
        num = (lm[0] + lm[1] + lm[2]) + 2.0 * (lm[3] + lm[4] + lm[5])
        den = (mm[0] + mm[1] + mm[2]) + 2.0 * (mm[3] + mm[4] + mm[5])
        return num, den

    def fold(value):
        parts = [value[:, k:k + 128] for k in range(0, value.shape[1], 128)]
        return functools.reduce(lambda x, y: x + y, parts)

    def sums(t, rows):
        both = [sums_row(t, row) for row in rows]
        num = functools.reduce(lambda x, y: x + y, [b[0] for b in both])
        den = functools.reduce(lambda x, y: x + y, [b[1] for b in both])
        accn[tile(t - 1), :] += fold(num)
        accd[tile(t - 1), :] += fold(den)

    def inner_filter(t, carry):
        span_rows(t, range(edge_lo, edge_hi + 1))
        filtered_rows(t, range(edge_lo + 1, edge_hi))
        return carry

    lax.fori_loop(1, nt + 1, inner_filter, 0)

    @pl.when(not_high)
    def _():
        y_copy(0).wait_recv()

    @pl.when(not_low)
    def _():
        y_copy(1).wait_recv()

    def end_filter(i, carry):
        return inner_filter(i * (nt + 1), carry)

    lax.fori_loop(0, 2, end_filter, 0)

    half = (nx - 2) // 2

    def inner_stress(i, carry):
        t = i // half + 1
        row = edge_lo + 1 + 2 * lax.rem(i, half)
        stress_row(t, row, True)
        stress_row(t, row + 1, True)
        return carry

    lax.fori_loop(0, nt * half, inner_stress, 0)
    close_round(0)
    open_round(1)

    @pl.when(begins)
    def _():
        pl.semaphore_wait(ready.at[1], 1)
        near_copy(0).start()

    def inner_sums(t, carry):
        sums(t, range(edge_lo + 2, edge_hi - 1))
        return carry

    lax.fori_loop(1, nt + 1, inner_sums, 0)
    close_round(1)
    open_round(2)

    for side in range(2):
        near_copy(side).wait_send()
        start_all(0, (side,))


    def step(side, k, t):
        new, middle, old = (halo_row(side, k - j) for j in range(3))
        span_rows(t, (new,), k == 1 or shifting and k == 2)
        filtered_rows(t, (middle,))
        stress_row(t, middle, k == 1)
        sums(t, (old,))

    for side in range(2):
        near_copy(1 - side).wait_recv()

        @pl.when(not_high)
        def _():
            c_copy(side, 1).start()

        @pl.when(not_low)
        def _():
            c_copy(side, 0).start()

    def near(i, carry):
        for side in range(2):
            step(side, 1, i)

        @pl.when(i == nt // 2)
        def _():
            start_all(1)

        return carry

    lax.fori_loop(1, nt + 1, near, 0)
    start_all(2)
    for side in range(2):
        start_moved(side)
    close_round(2)

    def later_round(k):
        open_round(k)
        close_round(k)

    for k in range(3, len(reaches)):
        later_round(k)
    to_ends(ring.at[len(reaches)])

    @pl.when(not_high)
    def _():
        c_all(0, 2, c_recv.at[0]).wait_recv()

    @pl.when(not_low)
    def _():
        c_all(1, 2, c_recv.at[1]).wait_recv()

    def corners(i, carry):
        t = i * (nt + 1)
        for side in range(2):
            span_rows(t, (halo_row(side, 1),), False)
            filtered_rows(t, (halo_row(side, 0),))
        return carry

    lax.fori_loop(0, 2, corners, 0)

    def far(p):
        def both(i, carry):
            for side in range(2):
                step(side, 2, order(i))
            return carry

        def one(side):
            def run(i, carry):
                step(side, 2, order(i))
                return carry

            return run

        if not shifting or p < pieces - amounts[-1]:
            for side in range(2):
                wait_far(side, p)
            lax.fori_loop(cuts[p], cuts[p + 1], both, 0)
            return
        for side in range(2):
            @pl.when(p < pieces + gains[side])
            def _():
                wait_far(side, p)
                lax.fori_loop(cuts[p], cuts[p + 1], one(side), 0)

    far(0)
    start_all(3)

    def column_sums(ref):
        ref[0:1, :] = jnp.sum(accn[...].T, axis=0, keepdims=True)
        ref[1:2, :] = jnp.sum(accd[...].T, axis=0, keepdims=True)

    def g_copy(kind, to_x, to_y):
        return pltpu.make_async_remote_copy(
            src_ref=mine if kind == 0 else mine_ends,
            dst_ref=gather.at[kind, gx],
            send_sem=g_send.at[kind],
            recv_sem=g_recv.at[kind],
            device_id=(to_x, to_y),
            device_id_type=MESH,
        )

    def g_all(kind):
        count = n - 1 if kind == 0 else n
        part = gather.at[kind, 0:count]
        return pltpu.make_async_remote_copy(
            src_ref=part,
            dst_ref=part,
            send_sem=g_send.at[kind],
            recv_sem=g_recv.at[kind],
            device_id=(right, gy),
            device_id_type=MESH,
        )

    column_sums(mine_ends)
    pl.semaphore_wait(ring.at[len(reaches)], ends)

    def send_ends(i, carry):
        @pl.when(not_low)
        def _():
            g_copy(2, i, gy - 1).start()

        @pl.when(not_high)
        def _():
            g_copy(1, i, gy + 1).start()

        return carry

    lax.fori_loop(0, n, send_ends, 0)

    for p in range(1, pieces):
        far(p)
        if p == 1:
            start_all(4)
    for side in range(2):
        def run(i, carry):
            step(side, 3, i)
            return carry

        for j in range(len(amounts)):
            @pl.when(gains[side] >= amounts[j])
            def _():
                moved_copy(1 - side, j).wait_recv()
                lax.fori_loop(*moved_tiles(j), run, 0)

    column_sums(mine)

    def send(i, carry):
        @pl.when(i != gx)
        def _():
            g_copy(0, i, gy).start()

        return carry

    lax.fori_loop(0, n, send, 0)
    gather[0, gx] = mine[...]
    drain()

    @pl.when(not_low)
    def _():
        c_all(0, nx + 2, c_recv.at[0]).wait_send()

    @pl.when(not_high)
    def _():
        c_all(1, nx + 2, c_recv.at[1]).wait_send()

    @pl.when(not_low)
    def _():
        g_all(2).wait_send()

    @pl.when(not_high)
    def _():
        g_all(1).wait_send()

    @pl.when(not_low)
    def _():
        g_all(1).wait_recv()

    @pl.when(not_high)
    def _():
        g_all(2).wait_recv()

    def profile(kind):
        total = functools.reduce(lambda x, y: x + y, [gather[kind, i] for i in range(n)])
        return jnp.clip(2.0 * (total[0:1] / total[1:2]), 0.0, clip_high)

    low_raw = pltpu.roll(profile(1), (lanes + 1 - ny) % lanes, 1)
    high_raw = pltpu.roll(profile(2), ny - 1, 1)
    g_all(0).wait_recv()
    raw = profile(0)
    where = lax.broadcasted_iota(jnp.int32, (1, lanes), 1)
    first = where == 0
    last = where == ny - 1
    under = jnp.where(first, raw, pltpu.roll(raw, 1, 1))
    over = jnp.where(last, raw, pltpu.roll(raw, lanes - 1, 1))
    under = jnp.where(jnp.logical_and(first, not_low), low_raw, under)
    over = jnp.where(jnp.logical_and(last, not_high), high_raw, over)
    coef_ref[...] = 0.25 * under + 0.5 * raw + 0.25 * over
    g_all(0).wait_send()


def local(n, m, shifts, velocity):
    _, nx, ny, nz = velocity.shape
    lanes = -(-ny // 128) * 128
    nt = ny // 8
    f32 = jnp.float32
    strength, coef = pl.pallas_call(
        functools.partial(kernel, n, m, nx, ny, shifts),
        out_shape=(
            jax.ShapeDtypeStruct((nx, ny, nz), f32),
            jax.ShapeDtypeStruct((1, lanes), f32),
        ),
        in_specs=[pl.BlockSpec(memory_space=pltpu.HBM)],
        out_specs=(
            pl.BlockSpec(memory_space=pltpu.VMEM),
            pl.BlockSpec(memory_space=pltpu.VMEM),
        ),
        scratch_shapes=[
            pltpu.VMEM((3, nx + 2 * HALO, ny + 16, nz), f32),
            pltpu.VMEM((3, nx + 2 * HALO, ny + 16, nz), f32),
            pltpu.VMEM((3, nx + 2 * HALO, ny + 16, nz), f32),
            pltpu.VMEM((3, nx + 2 * HALO, ny + 16, nz), f32),
            pltpu.VMEM((6, nx + 2 * HALO, ny, nz), f32),
            pltpu.VMEM((lanes, 128), f32),
            pltpu.VMEM((lanes, 128), f32),
            pltpu.VMEM((2, lanes), f32),
            pltpu.VMEM((2, lanes), f32),
            pltpu.VMEM((3, n, 2, lanes), f32),
            pltpu.SemaphoreType.DMA((3,)),
            pltpu.SemaphoreType.DMA((2,)),
            pltpu.SemaphoreType.DMA((2, len(cuts_of(nt)) + len(amounts_of(shifts)))),
            pltpu.SemaphoreType.DMA((2,)),
            pltpu.SemaphoreType.DMA((2,)),
            pltpu.SemaphoreType.DMA((2,)),
            pltpu.SemaphoreType.DMA((3,)),
            pltpu.SemaphoreType.DMA((3,)),
            pltpu.SemaphoreType.REGULAR((3,)),
            pltpu.SemaphoreType.REGULAR((n.bit_length() + 1,)),
        ],
        compiler_params=pltpu.CompilerParams(
            collective_id=0, has_side_effects=True, vmem_limit_bytes=32 * 1024 * 1024
        ),
    )(pltpu.with_memory_space_constraint(velocity, pltpu.HBM))
    smooth = coef[0, :ny]
    return (smooth, smooth[None, :, None] * strength)


def solution(mesh):
    n, m = mesh.shape["gx"], mesh.shape["gy"]
    shifts = (0,) * (n - 2) + (1, 2)
    return jax.shard_map(
        functools.partial(local, n, m, shifts),
        mesh=mesh,
        in_specs=(P(None, "gx", "gy", None),),
        out_specs=(P("gy"), P("gx", "gy", None)),
        check_vma=False,
    )
```

```python
import functools

import jax
import jax.numpy as jnp
from jax import lax
from jax.experimental import pallas as pl
from jax.experimental.pallas import tpu as pltpu
from jax.sharding import PartitionSpec as P

clip_high = 0.1
pairs = ((0, 0), (1, 1), (2, 2), (0, 1), (0, 2), (1, 2))
MESH = pl.DeviceIdType.MESH
HALO = 3


def tile(index):
    return pl.ds(pl.multiple_of(index * 8, 8), 8)


def roll_next(value):
    return pltpu.roll(value, value.shape[1] - 1, 1)


def roll_prev(value):
    return pltpu.roll(value, 1, 1)


def filter_span(value):
    return (roll_next(value) + roll_prev(value)) + 2.0 * value


def slope_span(value):
    return roll_next(value) - roll_prev(value)


def slope_wall(ref, comp, row, t, here):
    rows = lax.broadcasted_iota(jnp.int32, here.shape, 0)
    below = ref[comp, row, tile(t - 1), :]
    above = ref[comp, row, tile(t + 1), :]
    up = pltpu.roll(jnp.where(rows == 0, above, here), 7, 0)
    down = pltpu.roll(jnp.where(rows == 7, below, here), 1, 0)
    return up - down


def strain4(ref, row, t, slope=None):
    here = [ref[c, row, tile(t), :] for c in range(3)]
    dx = [ref[c, row + 1, tile(t), :] - ref[c, row - 1, tile(t), :] for c in range(3)]
    dy = [slope_wall(ref, c, row, t, here[c]) for c in range(3)]
    if slope is None:
        dz = [slope_span(here[c]) for c in range(3)]
    else:
        dz = [slope[c, row, tile(t), :] for c in range(3)]
    s = (
        dx[0],
        4.0 * dy[1],
        2.0 * dz[2],
        2.0 * dy[0] + 0.5 * dx[1],
        dz[0] + 0.5 * dx[2],
        dz[1] + 2.0 * dy[2],
    )
    diag = s[0] * s[0] + s[1] * s[1] + s[2] * s[2]
    off = s[3] * s[3] + s[4] * s[4] + s[5] * s[5]
    return here, s, diag + 2.0 * off


def cuts_of(nt):
    edges = [0, min(3, nt)]
    while nt - edges[-1] > 1:
        edges.append(min(edges[-1] + 2, nt - 1))
    if edges[-1] < nt:
        edges.append(nt)
    return edges


def amounts_of(shifts):
    return sorted({abs(s) for s in shifts} - {0})


def kernel(n, m, nx, ny, shifts, u_hbm, strength, coef_ref, u, w, v, d, g, accn, accd,
           mine, mine_ends, gather, own_sem, xs_send, xs_recv, y_send, y_recv,
           c_recv, g_send, g_recv, ready, ring):
    nt = ny // 8
    edge_lo, edge_hi = HALO, HALO + nx - 1
    gx = lax.axis_index("gx")
    gy = lax.axis_index("gy")
    left, right = lax.rem(gx + n - 1, n), lax.rem(gx + 1, n)
    not_low, not_high = gy > 0, gy < m - 1
    begins, closes = gx == 0, gx == n - 1
    lanes = mine.shape[-1]
    shifting = any(shifts)
    cuts = cuts_of(nt)
    pieces = len(cuts) - 1
    amounts = amounts_of(shifts)

    def shift_at(index):
        value = jnp.int32(shifts[0])
        for i in range(1, n):
            if shifts[i] != shifts[0]:
                value = jnp.where(index == i, jnp.int32(shifts[i]), value)
        return value

    gains = (shift_at(left), -shift_at(gx)) if shifting else (0, 0)

    own = [
        pltpu.make_async_copy(
            u_hbm.at[:, a:b, :, :], u.at[:, edge_lo + a:edge_lo + b, 8:8 + ny, :], own_sem.at[k]
        )
        for k, (a, b) in enumerate(((0, 1), (nx - 1, nx), (1, nx - 1)))
    ]
    for copy in own:
        copy.start()

    def signal(semaphore, to_x, to_y):
        pl.semaphore_signal(semaphore, inc=1, device_id=(to_x, to_y), device_id_type=MESH)

    barrier = pltpu.get_barrier_semaphore()

    even = lax.rem(gx, 2) == 0
    paired = jnp.logical_or(jnp.logical_not(even), gx < n - 1)
    waits_right = jnp.logical_and(jnp.logical_not(even), jnp.logical_not(closes))
    later_left = jnp.logical_and(even, gx > 0)

    @pl.when(paired)
    def _():
        signal(barrier, jnp.where(even, right, left), gy)

    @pl.when(waits_right)
    def _():
        signal(barrier, right, gy)

    @pl.when(begins)
    def _():
        signal(barrier, left, gy)

    @pl.when(not_high)
    def _():
        signal(barrier, gx, gy + 1)

    earlier = [jnp.where(x, 1, 0) for x in (paired, later_left, closes, not_low)]
    greeted = sum(earlier)

    @pl.when(greeted > 0)
    def _():
        pl.semaphore_wait(barrier, greeted)

    @pl.when(later_left)
    def _():
        signal(ready.at[0], left, gy)

    @pl.when(closes)
    def _():
        signal(ready.at[1], right, gy)

    @pl.when(not_low)
    def _():
        signal(ready.at[2], gx, gy - 1)

    ends = jnp.where(not_low, 1, 0) + jnp.where(not_high, 1, 0)
    reaches = [2 ** k for k in range(n.bit_length()) if 2 ** k < n]

    def open_round(k):
        if k < len(reaches):
            @pl.when(gx >= reaches[k])
            def _():
                signal(ring.at[k], gx - reaches[k], gy)

            @pl.when(gx < n - reaches[k])
            def _():
                signal(ring.at[k], gx + reaches[k], gy)

    def close_round(k):
        if k < len(reaches):
            near = (gx >= reaches[k], gx < n - reaches[k])
            count = jnp.where(near[0], 1, 0) + jnp.where(near[1], 1, 0)

            @pl.when(count > 0)
            def _():
                pl.semaphore_wait(ring.at[k], count)

    def to_ends(semaphore):
        @pl.when(not_low)
        def _():
            signal(semaphore, gx, gy - 1)

        @pl.when(not_high)
        def _():
            signal(semaphore, gx, gy + 1)

    def order(i):
        return jnp.where(i == 0, nt, i)

    def halo_row(side, k):
        return edge_lo - k if side == 0 else edge_hi + k

    def x_copy(side, k, low, high, slot):
        src = halo_row(side, 1 - k)
        dst = halo_row(1 - side, k)
        return pltpu.make_async_remote_copy(
            src_ref=u.at[:, src:src + 1, 8 * low:8 * high, :],
            dst_ref=u.at[:, dst:dst + 1, 8 * low:8 * high, :],
            send_sem=xs_send.at[side],
            recv_sem=xs_recv.at[1 - side, slot],
            device_id=(left if side == 0 else right, gy),
            device_id_type=MESH,
        )

    def near_copy(side):
        return x_copy(side, 1, 1, nt + 1, 0)

    def moved_tiles(j):
        high = pieces - amounts[j - 1] if j else pieces
        return cuts[pieces - amounts[j]], cuts[high]

    def moved_copy(side, j):
        return x_copy(side, 3, *moved_tiles(j), pieces + 1 + j)

    def far_parts(p):
        if p == 0:
            return [(nt, nt + 1), (1, cuts[1])] if cuts[1] > 1 else [(nt, nt + 1)]
        return [(cuts[p], cuts[p + 1])]

    def start_far(side, p):
        def run():
            for low, high in far_parts(p):
                x_copy(side, 2, low, high, p + 1).start()

        if shifting and p >= pieces - amounts[-1]:
            pl.when(p < pieces - gains[side])(run)
        else:
            run()

    def start_moved(side):
        for j in range(len(amounts)):
            @pl.when(gains[side] <= -amounts[j])
            def _():
                moved_copy(side, j).start()

    def wait_far(side, p):
        count = cuts[p + 1] - cuts[p]
        x_copy(1 - side, 2, 1, 1 + count, p + 1).wait_recv()

    def tiles_view(count):
        rows = next(r for r in range(1, u.shape[1] + 1) if count % r == 0 and count // r <= nt + 2)
        return u.at[:, 0:rows, 0:8 * (count // rows), :]

    def drain():
        for side in range(2):
            if not shifting:
                wait_rows(side, tiles_view(nt))
                continue
            kept = [cuts[pieces - a] for a in amounts]
            cases = [(0, nt)] + list(zip(amounts, kept)) + [(-a, 2 * nt - c) for a, c in zip(amounts, kept)]
            for gain, count in cases:
                @pl.when(gains[side] == gain)
                def _():
                    wait_rows(side, tiles_view(count))

    def y_copy(side):
        src = 8 if side == 0 else ny + 7
        dst = ny + 8 if side == 0 else 7
        return pltpu.make_async_remote_copy(
            src_ref=u.at[:, edge_lo:edge_lo + nx, src:src + 1, :],
            dst_ref=u.at[:, edge_lo:edge_lo + nx, dst:dst + 1, :],
            send_sem=y_send.at[side],
            recv_sem=y_recv.at[side],
            device_id=(gx, gy - 1 if side == 0 else gy + 1),
            device_id_type=MESH,
        )

    def c_copy(side, end):
        row = halo_row(side, 1)
        src = 8 if end == 0 else ny + 7
        dst = ny + 8 if end == 0 else 7
        return pltpu.make_async_remote_copy(
            src_ref=u.at[:, row:row + 1, src:src + 1, :],
            dst_ref=u.at[:, row:row + 1, dst:dst + 1, :],
            send_sem=y_send.at[end],
            recv_sem=c_recv.at[end],
            device_id=(gx, gy - 1 if end == 0 else gy + 1),
            device_id_type=MESH,
        )

    def c_all(end, rows, semaphore):
        part = u.at[:, 0:rows, 8:9, :]
        return pltpu.make_async_remote_copy(
            src_ref=part,
            dst_ref=part,
            send_sem=y_send.at[end],
            recv_sem=semaphore,
            device_id=(gx, gy - 1 if end == 0 else gy + 1),
            device_id_type=MESH,
        )

    def wait_rows(side, part):
        pltpu.make_async_remote_copy(
            src_ref=part,
            dst_ref=part,
            send_sem=xs_send.at[side],
            recv_sem=xs_recv.at[1 - side, 0],
            device_id=(left if side == 0 else right, gy),
            device_id_type=MESH,
        ).wait_send()

    plans = (((0, 1), (2, 3), (), (), ()), ((0,), (), (1, 2), (3,), ()))
    odd = lax.rem(gy, 2) == 1

    def start_all(point, sides=(0, 1)):
        chosen = [[p for p in plan[point] if p < pieces] for plan in plans]

        def run(parts):
            for p in parts:
                for side in sides:
                    start_far(side, p)

        if chosen[0] == chosen[1]:
            run(chosen[0])
            return
        if chosen[0]:
            pl.when(jnp.logical_not(odd))(lambda: run(chosen[0]))
        if chosen[1]:
            pl.when(odd)(lambda: run(chosen[1]))

    own[0].wait()

    @pl.when(gx > 0)
    def _():
        near_copy(0).start()

    own[1].wait()

    @pl.when(jnp.logical_not(waits_right))
    def _():
        near_copy(1).start()

    own[2].wait()

    @pl.when(not_low)
    def _():
        y_copy(0).start()

    @pl.when(waits_right)
    def _():
        pl.semaphore_wait(ready.at[0], 1)
        near_copy(1).start()

    open_round(0)

    @pl.when(not_high)
    def _():
        pl.semaphore_wait(ready.at[2], 1)
        y_copy(1).start()

    accn[...] = jnp.zeros_like(accn)
    accd[...] = jnp.zeros_like(accd)
    rows_all = u.shape[1]

    @pl.when(jnp.logical_not(not_low))
    def _():
        u[:, :, 0:8, :] = jnp.zeros((3, rows_all, 8, u.shape[3]), jnp.float32)

    @pl.when(jnp.logical_not(not_high))
    def _():
        u[:, :, ny + 8:ny + 16, :] = jnp.zeros((3, rows_all, 8, u.shape[3]), jnp.float32)

    def span_rows(t, rows, slopes=True):
        for c in range(3):
            for row in rows:
                here = u[c, row, tile(t), :]
                after, before = roll_next(here), roll_prev(here)
                w[c, row, tile(t), :] = (after + before) + 2.0 * here
                if slopes:
                    d[c, row, tile(t), :] = after - before

    def filtered_rows(t, rows):
        for c in range(3):
            for row in rows:
                a, b, e = (w[c, row + k, tile(t), :] for k in (-1, 0, 1))
                v[c, row, tile(t), :] = 0.25 * ((a + e) + 2.0 * b)

    def stress_row(t, row, keep):
        _, s, total = strain4(u, row, t, d)
        size = jnp.sqrt(0.125 * total)
        if keep:
            strength[row - edge_lo, tile(t - 1), :] = size
        for k in range(6):
            g[k, row, tile(t - 1), :] = size * s[k]

    def sums_row(t, row):
        centre, s, total = strain4(v, row, t)
        scale = jnp.sqrt(2.0 * total)

        def product(a, b):
            one, two, three = (near[j][a] * near[j][b] for j in range(3))
            return filter_span((one + three) + 2.0 * two)

        def stress(k):
            one, two, three = (g[k, row + j, tile(t - 1), :] for j in (-1, 0, 1))
            return filter_span((one + three) + 2.0 * two)

        near = [[u[c, row + j, tile(t), :] for c in range(3)] for j in (-1, 0, 1)]
        leonard = [product(a, b) - centre[a] * centre[b] for a, b in pairs]
        third = (leonard[0] + leonard[1] + leonard[2]) * (1.0 / 3.0)
        leonard = [x - third for x in leonard[:3]] + leonard[3:]
        model = [stress(k) - scale * s[k] for k in range(6)]
        lm = [x * y for x, y in zip(leonard, model)]
        mm = [x * x for x in model]
        num = (lm[0] + lm[1] + lm[2]) + 2.0 * (lm[3] + lm[4] + lm[5])
        den = (mm[0] + mm[1] + mm[2]) + 2.0 * (mm[3] + mm[4] + mm[5])
        return num, den

    def fold(value):
        parts = [value[:, k:k + 128] for k in range(0, value.shape[1], 128)]
        return functools.reduce(lambda x, y: x + y, parts)

    def sums(t, rows):
        both = [sums_row(t, row) for row in rows]
        num = functools.reduce(lambda x, y: x + y, [b[0] for b in both])
        den = functools.reduce(lambda x, y: x + y, [b[1] for b in both])
        accn[tile(t - 1), :] += fold(num)
        accd[tile(t - 1), :] += fold(den)

    def inner_filter(t, carry):
        span_rows(t, range(edge_lo, edge_hi + 1))
        filtered_rows(t, range(edge_lo + 1, edge_hi))
        return carry

    lax.fori_loop(1, nt + 1, inner_filter, 0)

    @pl.when(not_high)
    def _():
        y_copy(0).wait_recv()

    @pl.when(not_low)
    def _():
        y_copy(1).wait_recv()

    def end_filter(i, carry):
        return inner_filter(i * (nt + 1), carry)

    lax.fori_loop(0, 2, end_filter, 0)

    half = (nx - 2) // 2

    def inner_stress(i, carry):
        t = i // half + 1
        row = edge_lo + 1 + 2 * lax.rem(i, half)
        stress_row(t, row, True)
        stress_row(t, row + 1, True)
        return carry

    lax.fori_loop(0, nt * half, inner_stress, 0)
    close_round(0)
    open_round(1)

    @pl.when(begins)
    def _():
        pl.semaphore_wait(ready.at[1], 1)
        near_copy(0).start()

    def inner_sums(t, carry):
        sums(t, range(edge_lo + 2, edge_hi - 1))
        return carry

    lax.fori_loop(1, nt + 1, inner_sums, 0)
    close_round(1)
    open_round(2)

    for side in range(2):
        near_copy(side).wait_send()
        start_all(0, (side,))


    def step(side, k, t):
        new, middle, old = (halo_row(side, k - j) for j in range(3))
        span_rows(t, (new,), k == 1 or shifting and k == 2)
        filtered_rows(t, (middle,))
        stress_row(t, middle, k == 1)
        sums(t, (old,))

    for side in range(2):
        near_copy(1 - side).wait_recv()

        @pl.when(not_high)
        def _():
            c_copy(side, 1).start()

        @pl.when(not_low)
        def _():
            c_copy(side, 0).start()

    def near(i, carry):
        for side in range(2):
            step(side, 1, i)

        @pl.when(i == nt // 2)
        def _():
            start_all(1)

        return carry

    lax.fori_loop(1, nt + 1, near, 0)
    start_all(2)
    for side in range(2):
        start_moved(side)
    close_round(2)

    def later_round(k):
        open_round(k)
        close_round(k)

    for k in range(3, len(reaches)):
        later_round(k)
    to_ends(ring.at[len(reaches)])

    @pl.when(not_high)
    def _():
        c_all(0, 2, c_recv.at[0]).wait_recv()

    @pl.when(not_low)
    def _():
        c_all(1, 2, c_recv.at[1]).wait_recv()

    def corners(i, carry):
        t = i * (nt + 1)
        for side in range(2):
            span_rows(t, (halo_row(side, 1),), False)
            filtered_rows(t, (halo_row(side, 0),))
        return carry

    lax.fori_loop(0, 2, corners, 0)

    def far(p):
        def both(i, carry):
            for side in range(2):
                step(side, 2, order(i))
            return carry

        def one(side):
            def run(i, carry):
                step(side, 2, order(i))
                return carry

            return run

        if not shifting or p < pieces - amounts[-1]:
            for side in range(2):
                wait_far(side, p)
            lax.fori_loop(cuts[p], cuts[p + 1], both, 0)
            return
        for side in range(2):
            @pl.when(p < pieces + gains[side])
            def _():
                wait_far(side, p)
                lax.fori_loop(cuts[p], cuts[p + 1], one(side), 0)

    far(0)
    start_all(3)

    def column_sums(ref):
        ref[0:1, :] = jnp.sum(accn[...].T, axis=0, keepdims=True)
        ref[1:2, :] = jnp.sum(accd[...].T, axis=0, keepdims=True)

    def g_copy(kind, to_x, to_y):
        return pltpu.make_async_remote_copy(
            src_ref=mine if kind == 0 else mine_ends,
            dst_ref=gather.at[kind, gx],
            send_sem=g_send.at[kind],
            recv_sem=g_recv.at[kind],
            device_id=(to_x, to_y),
            device_id_type=MESH,
        )

    def g_all(kind):
        count = n - 1 if kind == 0 else n
        part = gather.at[kind, 0:count]
        return pltpu.make_async_remote_copy(
            src_ref=part,
            dst_ref=part,
            send_sem=g_send.at[kind],
            recv_sem=g_recv.at[kind],
            device_id=(right, gy),
            device_id_type=MESH,
        )

    column_sums(mine_ends)
    pl.semaphore_wait(ring.at[len(reaches)], ends)

    def send_ends(i, carry):
        @pl.when(not_low)
        def _():
            g_copy(2, i, gy - 1).start()

        @pl.when(not_high)
        def _():
            g_copy(1, i, gy + 1).start()

        return carry

    lax.fori_loop(0, n, send_ends, 0)

    for p in range(1, pieces):
        far(p)
        if p == 1:
            start_all(4)
    for side in range(2):
        def run(i, carry):
            step(side, 3, i)
            return carry

        for j in range(len(amounts)):
            @pl.when(gains[side] >= amounts[j])
            def _():
                moved_copy(1 - side, j).wait_recv()
                lax.fori_loop(*moved_tiles(j), run, 0)

    column_sums(mine)

    def send(i, carry):
        @pl.when(i != gx)
        def _():
            g_copy(0, i, gy).start()

        return carry

    lax.fori_loop(0, n, send, 0)
    gather[0, gx] = mine[...]
    drain()

    @pl.when(not_low)
    def _():
        c_all(0, nx + 2, c_recv.at[0]).wait_send()

    @pl.when(not_high)
    def _():
        c_all(1, nx + 2, c_recv.at[1]).wait_send()

    @pl.when(not_low)
    def _():
        g_all(2).wait_send()

    @pl.when(not_high)
    def _():
        g_all(1).wait_send()

    @pl.when(not_low)
    def _():
        g_all(1).wait_recv()

    @pl.when(not_high)
    def _():
        g_all(2).wait_recv()

    def profile(kind):
        total = functools.reduce(lambda x, y: x + y, [gather[kind, i] for i in range(n)])
        return jnp.clip(2.0 * (total[0:1] / total[1:2]), 0.0, clip_high)

    low_raw = pltpu.roll(profile(1), (lanes + 1 - ny) % lanes, 1)
    high_raw = pltpu.roll(profile(2), ny - 1, 1)
    g_all(0).wait_recv()
    raw = profile(0)
    where = lax.broadcasted_iota(jnp.int32, (1, lanes), 1)
    first = where == 0
    last = where == ny - 1
    under = jnp.where(first, raw, pltpu.roll(raw, 1, 1))
    over = jnp.where(last, raw, pltpu.roll(raw, lanes - 1, 1))
    under = jnp.where(jnp.logical_and(first, not_low), low_raw, under)
    over = jnp.where(jnp.logical_and(last, not_high), high_raw, over)
    coef_ref[...] = 0.25 * under + 0.5 * raw + 0.25 * over
    g_all(0).wait_send()


def local(n, m, shifts, velocity):
    _, nx, ny, nz = velocity.shape
    lanes = -(-ny // 128) * 128
    nt = ny // 8
    f32 = jnp.float32
    strength, coef = pl.pallas_call(
        functools.partial(kernel, n, m, nx, ny, shifts),
        out_shape=(
            jax.ShapeDtypeStruct((nx, ny, nz), f32),
            jax.ShapeDtypeStruct((1, lanes), f32),
        ),
        in_specs=[pl.BlockSpec(memory_space=pltpu.HBM)],
        out_specs=(
            pl.BlockSpec(memory_space=pltpu.VMEM),
            pl.BlockSpec(memory_space=pltpu.VMEM),
        ),
        scratch_shapes=[
            pltpu.VMEM((3, nx + 2 * HALO, ny + 16, nz), f32),
            pltpu.VMEM((3, nx + 2 * HALO, ny + 16, nz), f32),
            pltpu.VMEM((3, nx + 2 * HALO, ny + 16, nz), f32),
            pltpu.VMEM((3, nx + 2 * HALO, ny + 16, nz), f32),
            pltpu.VMEM((6, nx + 2 * HALO, ny, nz), f32),
            pltpu.VMEM((lanes, 128), f32),
            pltpu.VMEM((lanes, 128), f32),
            pltpu.VMEM((2, lanes), f32),
            pltpu.VMEM((2, lanes), f32),
            pltpu.VMEM((3, n, 2, lanes), f32),
            pltpu.SemaphoreType.DMA((3,)),
            pltpu.SemaphoreType.DMA((2,)),
            pltpu.SemaphoreType.DMA((2, len(cuts_of(nt)) + len(amounts_of(shifts)))),
            pltpu.SemaphoreType.DMA((2,)),
            pltpu.SemaphoreType.DMA((2,)),
            pltpu.SemaphoreType.DMA((2,)),
            pltpu.SemaphoreType.DMA((3,)),
            pltpu.SemaphoreType.DMA((3,)),
            pltpu.SemaphoreType.REGULAR((3,)),
            pltpu.SemaphoreType.REGULAR((n.bit_length() + 1,)),
        ],
        compiler_params=pltpu.CompilerParams(
            collective_id=0, has_side_effects=True, vmem_limit_bytes=32 * 1024 * 1024
        ),
    )(pltpu.with_memory_space_constraint(velocity, pltpu.HBM))
    smooth = coef[0, :ny]
    return (smooth, smooth[None, :, None] * strength)


def solution(mesh):
    n, m = mesh.shape["gx"], mesh.shape["gy"]
    shifts = (0,) * (n - 2) + (1, 2)
    return jax.shard_map(
        functools.partial(local, n, m, shifts),
        mesh=mesh,
        in_specs=(P(None, "gx", "gy", None),),
        out_specs=(P("gy"), P("gx", "gy", None)),
        check_vma=False,
    )
```

```python
import functools

import jax
import jax.numpy as jnp
from jax import lax
from jax.experimental import pallas as pl
from jax.experimental.pallas import tpu as pltpu
from jax.sharding import PartitionSpec as P

clip_high = 0.1
pairs = ((0, 0), (1, 1), (2, 2), (0, 1), (0, 2), (1, 2))
MESH = pl.DeviceIdType.MESH
HALO = 3


def tile(index):
    return pl.ds(pl.multiple_of(index * 8, 8), 8)


def roll_next(value):
    return pltpu.roll(value, value.shape[1] - 1, 1)


def roll_prev(value):
    return pltpu.roll(value, 1, 1)


def filter_span(value):
    return (roll_next(value) + roll_prev(value)) + 2.0 * value


def slope_span(value):
    return roll_next(value) - roll_prev(value)


def slope_wall(ref, comp, row, t, here):
    rows = lax.broadcasted_iota(jnp.int32, here.shape, 0)
    below = ref[comp, row, tile(t - 1), :]
    above = ref[comp, row, tile(t + 1), :]
    up = pltpu.roll(jnp.where(rows == 0, above, here), 7, 0)
    down = pltpu.roll(jnp.where(rows == 7, below, here), 1, 0)
    return up - down


def strain4(ref, row, t, slope=None):
    here = [ref[c, row, tile(t), :] for c in range(3)]
    dx = [ref[c, row + 1, tile(t), :] - ref[c, row - 1, tile(t), :] for c in range(3)]
    dy = [slope_wall(ref, c, row, t, here[c]) for c in range(3)]
    if slope is None:
        dz = [slope_span(here[c]) for c in range(3)]
    else:
        dz = [slope[c, row, tile(t), :] for c in range(3)]
    s = (
        dx[0],
        4.0 * dy[1],
        2.0 * dz[2],
        2.0 * dy[0] + 0.5 * dx[1],
        dz[0] + 0.5 * dx[2],
        dz[1] + 2.0 * dy[2],
    )
    diag = s[0] * s[0] + s[1] * s[1] + s[2] * s[2]
    off = s[3] * s[3] + s[4] * s[4] + s[5] * s[5]
    return here, s, diag + 2.0 * off


def cuts_of(nt):
    edges = [0, min(3, nt)]
    while nt - edges[-1] > 1:
        edges.append(min(edges[-1] + 2, nt - 1))
    if edges[-1] < nt:
        edges.append(nt)
    return edges


def amounts_of(shifts):
    return sorted({abs(s) for s in shifts} - {0})


def kernel(n, m, nx, ny, shifts, u_hbm, strength, coef_ref, u, w, v, d, g, accn, accd,
           mine, mine_ends, gather, own_sem, xs_send, xs_recv, y_send, y_recv,
           c_recv, g_send, g_recv, ready, ring):
    nt = ny // 8
    edge_lo, edge_hi = HALO, HALO + nx - 1
    gx = lax.axis_index("gx")
    gy = lax.axis_index("gy")
    left, right = lax.rem(gx + n - 1, n), lax.rem(gx + 1, n)
    not_low, not_high = gy > 0, gy < m - 1
    begins, closes = gx == 0, gx == n - 1
    lanes = mine.shape[-1]
    shifting = any(shifts)
    cuts = cuts_of(nt)
    pieces = len(cuts) - 1
    amounts = amounts_of(shifts)

    def shift_at(index):
        value = jnp.int32(shifts[0])
        for i in range(1, n):
            if shifts[i] != shifts[0]:
                value = jnp.where(index == i, jnp.int32(shifts[i]), value)
        return value

    gains = (shift_at(left), -shift_at(gx)) if shifting else (0, 0)

    own = [
        pltpu.make_async_copy(
            u_hbm.at[:, a:b, :, :], u.at[:, edge_lo + a:edge_lo + b, 8:8 + ny, :], own_sem.at[k]
        )
        for k, (a, b) in enumerate(((0, 1), (nx - 1, nx), (1, nx - 1)))
    ]
    for copy in own:
        copy.start()

    def signal(semaphore, to_x, to_y):
        pl.semaphore_signal(semaphore, inc=1, device_id=(to_x, to_y), device_id_type=MESH)

    barrier = pltpu.get_barrier_semaphore()

    even = lax.rem(gx, 2) == 0
    paired = jnp.logical_or(jnp.logical_not(even), gx < n - 1)
    waits_right = jnp.logical_and(jnp.logical_not(even), jnp.logical_not(closes))
    later_left = jnp.logical_and(even, gx > 0)

    @pl.when(paired)
    def _():
        signal(barrier, jnp.where(even, right, left), gy)

    @pl.when(waits_right)
    def _():
        signal(barrier, right, gy)

    @pl.when(begins)
    def _():
        signal(barrier, left, gy)

    @pl.when(not_high)
    def _():
        signal(barrier, gx, gy + 1)

    earlier = [jnp.where(x, 1, 0) for x in (paired, later_left, closes, not_low)]
    greeted = sum(earlier)

    @pl.when(greeted > 0)
    def _():
        pl.semaphore_wait(barrier, greeted)

    @pl.when(later_left)
    def _():
        signal(ready.at[0], left, gy)

    @pl.when(closes)
    def _():
        signal(ready.at[1], right, gy)

    @pl.when(not_low)
    def _():
        signal(ready.at[2], gx, gy - 1)

    ends = jnp.where(not_low, 1, 0) + jnp.where(not_high, 1, 0)
    reaches = [2 ** k for k in range(n.bit_length()) if 2 ** k < n]

    def open_round(k):
        if k < len(reaches):
            @pl.when(gx >= reaches[k])
            def _():
                signal(ring.at[k], gx - reaches[k], gy)

            @pl.when(gx < n - reaches[k])
            def _():
                signal(ring.at[k], gx + reaches[k], gy)

    def close_round(k):
        if k < len(reaches):
            near = (gx >= reaches[k], gx < n - reaches[k])
            count = jnp.where(near[0], 1, 0) + jnp.where(near[1], 1, 0)

            @pl.when(count > 0)
            def _():
                pl.semaphore_wait(ring.at[k], count)

    def to_ends(semaphore):
        @pl.when(not_low)
        def _():
            signal(semaphore, gx, gy - 1)

        @pl.when(not_high)
        def _():
            signal(semaphore, gx, gy + 1)

    def order(i):
        return jnp.where(i == 0, nt, i)

    def halo_row(side, k):
        return edge_lo - k if side == 0 else edge_hi + k

    def x_copy(side, k, low, high, slot):
        src = halo_row(side, 1 - k)
        dst = halo_row(1 - side, k)
        return pltpu.make_async_remote_copy(
            src_ref=u.at[:, src:src + 1, 8 * low:8 * high, :],
            dst_ref=u.at[:, dst:dst + 1, 8 * low:8 * high, :],
            send_sem=xs_send.at[side],
            recv_sem=xs_recv.at[1 - side, slot],
            device_id=(left if side == 0 else right, gy),
            device_id_type=MESH,
        )

    def near_copy(side):
        return x_copy(side, 1, 1, nt + 1, 0)

    def moved_tiles(j):
        high = pieces - amounts[j - 1] if j else pieces
        return cuts[pieces - amounts[j]], cuts[high]

    def moved_copy(side, j):
        return x_copy(side, 3, *moved_tiles(j), pieces + 1 + j)

    def far_parts(p):
        if p == 0:
            return [(nt, nt + 1), (1, cuts[1])] if cuts[1] > 1 else [(nt, nt + 1)]
        return [(cuts[p], cuts[p + 1])]

    def start_far(side, p):
        def run():
            for low, high in far_parts(p):
                x_copy(side, 2, low, high, p + 1).start()

        if shifting and p >= pieces - amounts[-1]:
            pl.when(p < pieces - gains[side])(run)
        else:
            run()

    def start_moved(side):
        for j in range(len(amounts)):
            @pl.when(gains[side] <= -amounts[j])
            def _():
                moved_copy(side, j).start()

    def wait_far(side, p):
        count = cuts[p + 1] - cuts[p]
        x_copy(1 - side, 2, 1, 1 + count, p + 1).wait_recv()

    def tiles_view(count):
        rows = next(r for r in range(1, u.shape[1] + 1) if count % r == 0 and count // r <= nt + 2)
        return u.at[:, 0:rows, 0:8 * (count // rows), :]

    def drain():
        for side in range(2):
            if not shifting:
                wait_rows(side, tiles_view(nt))
                continue
            kept = [cuts[pieces - a] for a in amounts]
            cases = [(0, nt)] + list(zip(amounts, kept)) + [(-a, 2 * nt - c) for a, c in zip(amounts, kept)]
            for gain, count in cases:
                @pl.when(gains[side] == gain)
                def _():
                    wait_rows(side, tiles_view(count))

    def y_copy(side):
        src = 8 if side == 0 else ny + 7
        dst = ny + 8 if side == 0 else 7
        return pltpu.make_async_remote_copy(
            src_ref=u.at[:, edge_lo:edge_lo + nx, src:src + 1, :],
            dst_ref=u.at[:, edge_lo:edge_lo + nx, dst:dst + 1, :],
            send_sem=y_send.at[side],
            recv_sem=y_recv.at[side],
            device_id=(gx, gy - 1 if side == 0 else gy + 1),
            device_id_type=MESH,
        )

    def c_copy(side, end):
        row = halo_row(side, 1)
        src = 8 if end == 0 else ny + 7
        dst = ny + 8 if end == 0 else 7
        return pltpu.make_async_remote_copy(
            src_ref=u.at[:, row:row + 1, src:src + 1, :],
            dst_ref=u.at[:, row:row + 1, dst:dst + 1, :],
            send_sem=y_send.at[end],
            recv_sem=c_recv.at[end],
            device_id=(gx, gy - 1 if end == 0 else gy + 1),
            device_id_type=MESH,
        )

    def c_all(end, rows, semaphore):
        part = u.at[:, 0:rows, 8:9, :]
        return pltpu.make_async_remote_copy(
            src_ref=part,
            dst_ref=part,
            send_sem=y_send.at[end],
            recv_sem=semaphore,
            device_id=(gx, gy - 1 if end == 0 else gy + 1),
            device_id_type=MESH,
        )

    def wait_rows(side, part):
        pltpu.make_async_remote_copy(
            src_ref=part,
            dst_ref=part,
            send_sem=xs_send.at[side],
            recv_sem=xs_recv.at[1 - side, 0],
            device_id=(left if side == 0 else right, gy),
            device_id_type=MESH,
        ).wait_send()

    plans = (((0, 1, 2), (3,), (), (), ()), ((0,), (), (1, 2), (3,), ()))
    odd = lax.rem(gy, 2) == 1

    def start_all(point, sides=(0, 1)):
        chosen = [[p for p in plan[point] if p < pieces] for plan in plans]

        def run(parts):
            for p in parts:
                for side in sides:
                    start_far(side, p)

        if chosen[0] == chosen[1]:
            run(chosen[0])
            return
        if chosen[0]:
            pl.when(jnp.logical_not(odd))(lambda: run(chosen[0]))
        if chosen[1]:
            pl.when(odd)(lambda: run(chosen[1]))

    own[0].wait()

    @pl.when(gx > 0)
    def _():
        near_copy(0).start()

    own[1].wait()

    @pl.when(jnp.logical_not(waits_right))
    def _():
        near_copy(1).start()

    own[2].wait()

    @pl.when(not_low)
    def _():
        y_copy(0).start()

    @pl.when(waits_right)
    def _():
        pl.semaphore_wait(ready.at[0], 1)
        near_copy(1).start()

    open_round(0)

    @pl.when(not_high)
    def _():
        pl.semaphore_wait(ready.at[2], 1)
        y_copy(1).start()

    accn[...] = jnp.zeros_like(accn)
    accd[...] = jnp.zeros_like(accd)
    rows_all = u.shape[1]

    @pl.when(jnp.logical_not(not_low))
    def _():
        u[:, :, 0:8, :] = jnp.zeros((3, rows_all, 8, u.shape[3]), jnp.float32)

    @pl.when(jnp.logical_not(not_high))
    def _():
        u[:, :, ny + 8:ny + 16, :] = jnp.zeros((3, rows_all, 8, u.shape[3]), jnp.float32)

    def span_rows(t, rows, slopes=True):
        for c in range(3):
            for row in rows:
                here = u[c, row, tile(t), :]
                after, before = roll_next(here), roll_prev(here)
                w[c, row, tile(t), :] = (after + before) + 2.0 * here
                if slopes:
                    d[c, row, tile(t), :] = after - before

    def filtered_rows(t, rows):
        for c in range(3):
            for row in rows:
                a, b, e = (w[c, row + k, tile(t), :] for k in (-1, 0, 1))
                v[c, row, tile(t), :] = 0.25 * ((a + e) + 2.0 * b)

    def stress_row(t, row, keep):
        _, s, total = strain4(u, row, t, d)
        size = jnp.sqrt(0.125 * total)
        if keep:
            strength[row - edge_lo, tile(t - 1), :] = size
        for k in range(6):
            g[k, row, tile(t - 1), :] = size * s[k]

    def sums_row(t, row):
        centre, s, total = strain4(v, row, t)
        scale = jnp.sqrt(2.0 * total)

        def product(a, b):
            one, two, three = (near[j][a] * near[j][b] for j in range(3))
            return filter_span((one + three) + 2.0 * two)

        def stress(k):
            one, two, three = (g[k, row + j, tile(t - 1), :] for j in (-1, 0, 1))
            return filter_span((one + three) + 2.0 * two)

        near = [[u[c, row + j, tile(t), :] for c in range(3)] for j in (-1, 0, 1)]
        leonard = [product(a, b) - centre[a] * centre[b] for a, b in pairs]
        third = (leonard[0] + leonard[1] + leonard[2]) * (1.0 / 3.0)
        leonard = [x - third for x in leonard[:3]] + leonard[3:]
        model = [stress(k) - scale * s[k] for k in range(6)]
        lm = [x * y for x, y in zip(leonard, model)]
        mm = [x * x for x in model]
        num = (lm[0] + lm[1] + lm[2]) + 2.0 * (lm[3] + lm[4] + lm[5])
        den = (mm[0] + mm[1] + mm[2]) + 2.0 * (mm[3] + mm[4] + mm[5])
        return num, den

    def fold(value):
        parts = [value[:, k:k + 128] for k in range(0, value.shape[1], 128)]
        return functools.reduce(lambda x, y: x + y, parts)

    def sums(t, rows):
        both = [sums_row(t, row) for row in rows]
        num = functools.reduce(lambda x, y: x + y, [b[0] for b in both])
        den = functools.reduce(lambda x, y: x + y, [b[1] for b in both])
        accn[tile(t - 1), :] += fold(num)
        accd[tile(t - 1), :] += fold(den)

    def inner_filter(t, carry):
        span_rows(t, range(edge_lo, edge_hi + 1))
        filtered_rows(t, range(edge_lo + 1, edge_hi))
        return carry

    lax.fori_loop(1, nt + 1, inner_filter, 0)

    @pl.when(not_high)
    def _():
        y_copy(0).wait_recv()

    @pl.when(not_low)
    def _():
        y_copy(1).wait_recv()

    def end_filter(i, carry):
        return inner_filter(i * (nt + 1), carry)

    lax.fori_loop(0, 2, end_filter, 0)

    half = (nx - 2) // 2

    def inner_stress(i, carry):
        t = i // half + 1
        row = edge_lo + 1 + 2 * lax.rem(i, half)
        stress_row(t, row, True)
        stress_row(t, row + 1, True)
        return carry

    lax.fori_loop(0, nt * half, inner_stress, 0)
    close_round(0)
    open_round(1)

    @pl.when(begins)
    def _():
        pl.semaphore_wait(ready.at[1], 1)
        near_copy(0).start()

    def inner_sums(t, carry):
        sums(t, range(edge_lo + 2, edge_hi - 1))
        return carry

    lax.fori_loop(1, nt + 1, inner_sums, 0)
    close_round(1)
    open_round(2)

    for side in range(2):
        near_copy(side).wait_send()
        start_all(0, (side,))


    def step(side, k, t):
        new, middle, old = (halo_row(side, k - j) for j in range(3))
        span_rows(t, (new,), k == 1 or shifting and k == 2)
        filtered_rows(t, (middle,))
        stress_row(t, middle, k == 1)
        sums(t, (old,))

    for side in range(2):
        near_copy(1 - side).wait_recv()

        @pl.when(not_high)
        def _():
            c_copy(side, 1).start()

        @pl.when(not_low)
        def _():
            c_copy(side, 0).start()

    def near(i, carry):
        for side in range(2):
            step(side, 1, i)

        @pl.when(i == nt // 2)
        def _():
            start_all(1)

        return carry

    lax.fori_loop(1, nt + 1, near, 0)
    start_all(2)
    for side in range(2):
        start_moved(side)
    close_round(2)

    def later_round(k):
        open_round(k)
        close_round(k)

    for k in range(3, len(reaches)):
        later_round(k)
    to_ends(ring.at[len(reaches)])

    @pl.when(not_high)
    def _():
        c_all(0, 2, c_recv.at[0]).wait_recv()

    @pl.when(not_low)
    def _():
        c_all(1, 2, c_recv.at[1]).wait_recv()

    def corners(i, carry):
        t = i * (nt + 1)
        for side in range(2):
            span_rows(t, (halo_row(side, 1),), False)
            filtered_rows(t, (halo_row(side, 0),))
        return carry

    lax.fori_loop(0, 2, corners, 0)

    def far(p):
        def both(i, carry):
            for side in range(2):
                step(side, 2, order(i))
            return carry

        def one(side):
            def run(i, carry):
                step(side, 2, order(i))
                return carry

            return run

        if not shifting or p < pieces - amounts[-1]:
            for side in range(2):
                wait_far(side, p)
            lax.fori_loop(cuts[p], cuts[p + 1], both, 0)
            return
        for side in range(2):
            @pl.when(p < pieces + gains[side])
            def _():
                wait_far(side, p)
                lax.fori_loop(cuts[p], cuts[p + 1], one(side), 0)

    far(0)
    start_all(3)

    def column_sums(ref):
        ref[0:1, :] = jnp.sum(accn[...].T, axis=0, keepdims=True)
        ref[1:2, :] = jnp.sum(accd[...].T, axis=0, keepdims=True)

    def g_copy(kind, to_x, to_y):
        return pltpu.make_async_remote_copy(
            src_ref=mine if kind == 0 else mine_ends,
            dst_ref=gather.at[kind, gx],
            send_sem=g_send.at[kind],
            recv_sem=g_recv.at[kind],
            device_id=(to_x, to_y),
            device_id_type=MESH,
        )

    def g_all(kind):
        count = n - 1 if kind == 0 else n
        part = gather.at[kind, 0:count]
        return pltpu.make_async_remote_copy(
            src_ref=part,
            dst_ref=part,
            send_sem=g_send.at[kind],
            recv_sem=g_recv.at[kind],
            device_id=(right, gy),
            device_id_type=MESH,
        )

    column_sums(mine_ends)
    pl.semaphore_wait(ring.at[len(reaches)], ends)

    def send_ends(i, carry):
        @pl.when(not_low)
        def _():
            g_copy(2, i, gy - 1).start()

        @pl.when(not_high)
        def _():
            g_copy(1, i, gy + 1).start()

        return carry

    lax.fori_loop(0, n, send_ends, 0)

    for p in range(1, pieces):
        far(p)
        if p == 1:
            start_all(4)
    for side in range(2):
        def run(i, carry):
            step(side, 3, i)
            return carry

        for j in range(len(amounts)):
            @pl.when(gains[side] >= amounts[j])
            def _():
                moved_copy(1 - side, j).wait_recv()
                lax.fori_loop(*moved_tiles(j), run, 0)

    column_sums(mine)

    def send(i, carry):
        @pl.when(i != gx)
        def _():
            g_copy(0, i, gy).start()

        return carry

    lax.fori_loop(0, n, send, 0)
    gather[0, gx] = mine[...]
    drain()

    @pl.when(not_low)
    def _():
        c_all(0, nx + 2, c_recv.at[0]).wait_send()

    @pl.when(not_high)
    def _():
        c_all(1, nx + 2, c_recv.at[1]).wait_send()

    @pl.when(not_low)
    def _():
        g_all(2).wait_send()

    @pl.when(not_high)
    def _():
        g_all(1).wait_send()

    @pl.when(not_low)
    def _():
        g_all(1).wait_recv()

    @pl.when(not_high)
    def _():
        g_all(2).wait_recv()

    def profile(kind):
        total = functools.reduce(lambda x, y: x + y, [gather[kind, i] for i in range(n)])
        return jnp.clip(2.0 * (total[0:1] / total[1:2]), 0.0, clip_high)

    low_raw = pltpu.roll(profile(1), (lanes + 1 - ny) % lanes, 1)
    high_raw = pltpu.roll(profile(2), ny - 1, 1)
    g_all(0).wait_recv()
    raw = profile(0)
    where = lax.broadcasted_iota(jnp.int32, (1, lanes), 1)
    first = where == 0
    last = where == ny - 1
    under = jnp.where(first, raw, pltpu.roll(raw, 1, 1))
    over = jnp.where(last, raw, pltpu.roll(raw, lanes - 1, 1))
    under = jnp.where(jnp.logical_and(first, not_low), low_raw, under)
    over = jnp.where(jnp.logical_and(last, not_high), high_raw, over)
    coef_ref[...] = 0.25 * under + 0.5 * raw + 0.25 * over
    g_all(0).wait_send()


def local(n, m, shifts, velocity):
    _, nx, ny, nz = velocity.shape
    lanes = -(-ny // 128) * 128
    nt = ny // 8
    f32 = jnp.float32
    strength, coef = pl.pallas_call(
        functools.partial(kernel, n, m, nx, ny, shifts),
        out_shape=(
            jax.ShapeDtypeStruct((nx, ny, nz), f32),
            jax.ShapeDtypeStruct((1, lanes), f32),
        ),
        in_specs=[pl.BlockSpec(memory_space=pltpu.HBM)],
        out_specs=(
            pl.BlockSpec(memory_space=pltpu.VMEM),
            pl.BlockSpec(memory_space=pltpu.VMEM),
        ),
        scratch_shapes=[
            pltpu.VMEM((3, nx + 2 * HALO, ny + 16, nz), f32),
            pltpu.VMEM((3, nx + 2 * HALO, ny + 16, nz), f32),
            pltpu.VMEM((3, nx + 2 * HALO, ny + 16, nz), f32),
            pltpu.VMEM((3, nx + 2 * HALO, ny + 16, nz), f32),
            pltpu.VMEM((6, nx + 2 * HALO, ny, nz), f32),
            pltpu.VMEM((lanes, 128), f32),
            pltpu.VMEM((lanes, 128), f32),
            pltpu.VMEM((2, lanes), f32),
            pltpu.VMEM((2, lanes), f32),
            pltpu.VMEM((3, n, 2, lanes), f32),
            pltpu.SemaphoreType.DMA((3,)),
            pltpu.SemaphoreType.DMA((2,)),
            pltpu.SemaphoreType.DMA((2, len(cuts_of(nt)) + len(amounts_of(shifts)))),
            pltpu.SemaphoreType.DMA((2,)),
            pltpu.SemaphoreType.DMA((2,)),
            pltpu.SemaphoreType.DMA((2,)),
            pltpu.SemaphoreType.DMA((3,)),
            pltpu.SemaphoreType.DMA((3,)),
            pltpu.SemaphoreType.REGULAR((3,)),
            pltpu.SemaphoreType.REGULAR((n.bit_length() + 1,)),
        ],
        compiler_params=pltpu.CompilerParams(
            collective_id=0, has_side_effects=True, vmem_limit_bytes=32 * 1024 * 1024
        ),
    )(pltpu.with_memory_space_constraint(velocity, pltpu.HBM))
    smooth = coef[0, :ny]
    return (smooth, smooth[None, :, None] * strength)


def solution(mesh):
    n, m = mesh.shape["gx"], mesh.shape["gy"]
    shifts = (0,) * (n - 2) + (1, 2)
    return jax.shard_map(
        functools.partial(local, n, m, shifts),
        mesh=mesh,
        in_specs=(P(None, "gx", "gy", None),),
        out_specs=(P("gy"), P("gx", "gy", None)),
        check_vma=False,
    )
```
